32 devices in a mesh: ta: 4 (over z), gz: 2 (over x), gy: 4 (over y, core).
Axes of the slice: x: 2, y: 2, z: 4, core: 2. Of those that a mesh axis runs over, the one named last changes fastest.
Arguments:
- lattice_links: float32 [2, 4, 18, 8, 16, 1024], P(None, None, None, 'ta', 'gz', 'gy'), may hold values from -1 to 1, as said below
- transform: float32 [2, 18, 8, 16, 1024], P(None, None, 'ta', 'gz', 'gy'), may hold values from -1 to 1, as said below
Outputs:
- fixed_transform: float32 [2, 18, 8, 16, 1024], P(None, None, 'ta', 'gz', 'gy')
- monitor: float32 [2, 2], replicated
The draws below stay inside these ranges and needn't reach their ends.
Inputs may be any that keep to these rules, and one draw needn't show every extreme that they name: `lattice_links`: every site's matrix for every colour and direction is special unitary. `transform`: every site's matrix is special unitary.
All inputs are finite; a program needn't handle non-finite values.
Results may differ from the reference program's by a relative error of at most 0.0003.
Values sent between devices are 32-bit elements; how exact they have to be, the bound alone decides.
A program may use at most 128 MiB of HBM per device.

```python
import math
import jax
import jax.numpy as jnp

NX = 64
ITERS = 2
NT = 8
NZ = 16
NY = 32


def turn_rows(mat_re, mat_im, quat, row_one, row_two):
    q_zero, q_one, q_two, q_three = quat
    upper_re, upper_im = (mat_re[row_one], mat_im[row_one])
    lower_re, lower_im = (mat_re[row_two], mat_im[row_two])
    top_re = q_zero * upper_re - q_three * upper_im + q_two * lower_re - q_one * lower_im
    top_im = q_zero * upper_im + q_three * upper_re + q_two * lower_im + q_one * lower_re
    bottom_re = -q_two * upper_re - q_one * upper_im + q_zero * lower_re + q_three * lower_im
    bottom_im = -q_two * upper_im + q_one * upper_re + q_zero * lower_im - q_three * lower_re
    rows_re = [mat_re[0], mat_re[1], mat_re[2]]
    rows_im = [mat_im[0], mat_im[1], mat_im[2]]
    rows_re[row_one] = top_re
    rows_im[row_one] = top_im
    rows_re[row_two] = bottom_re
    rows_im[row_two] = bottom_im
    return (jnp.stack(rows_re, 0), jnp.stack(rows_im, 0))


def special_unitary(key, lead, spread):
    ones = (1,) * len(lead)
    identity = jnp.eye(3, dtype=jnp.float32).reshape((3, 3) + ones)
    mat_re = identity + jnp.zeros((3, 3) + lead, jnp.float32)
    mat_im = jnp.zeros((3, 3) + lead, jnp.float32)
    pairs = ((0, 1), (0, 2), (1, 2), (0, 1), (0, 2), (1, 2))
    for number in range(6):
        keys = jax.random.split(jax.random.fold_in(key, number), 3)
        spread_angle = spread * jax.random.normal(keys[0], lead, jnp.float32)
        phase_one = math.pi * jax.random.uniform(keys[1], lead, jnp.float32, -1.0, 1.0)
        phase_two = math.pi * jax.random.uniform(keys[2], lead, jnp.float32, -1.0, 1.0)
        cos_a = jnp.cos(spread_angle)
        sin_a = jnp.sin(spread_angle)
        quat = (cos_a * jnp.cos(phase_one), cos_a * jnp.sin(phase_one), sin_a * jnp.cos(phase_two), sin_a * jnp.sin(phase_two))
        row_one, row_two = pairs[number]
        mat_re, mat_im = turn_rows(mat_re, mat_im, quat, row_one, row_two)
    return (mat_re, mat_im)


def draw_lattice_links(key, part):
    row_len = NY * NX // 2
    times = jnp.arange(NT, dtype=jnp.float32).reshape((1, 1, NT, 1, 1)) / NT
    spread = 0.4 + 0.8 * times
    mat_re, mat_im = special_unitary(jax.random.fold_in(key, 17), (2, 4, NT, NZ, row_len), spread)
    stacked = jnp.stack([mat_re, mat_im], 0)
    stacked = jnp.transpose(stacked, (3, 4, 0, 1, 2, 5, 6, 7))
    return stacked.reshape((2, 4, 18, NT, NZ, row_len)).astype(jnp.float32)


def draw_transform(key, part):
    row_len = NY * NX // 2
    times = jnp.arange(NT, dtype=jnp.float32).reshape((1, NT, 1, 1)) / NT
    spread = 0.3 + 0.9 * times
    mat_re, mat_im = special_unitary(jax.random.fold_in(key, 29), (2, NT, NZ, row_len), spread)
    stacked = jnp.stack([mat_re, mat_im], 0)
    stacked = jnp.transpose(stacked, (3, 0, 1, 2, 4, 5, 6))
    return stacked.reshape((2, 18, NT, NZ, row_len)).astype(jnp.float32)


def setup_inputs(seed: int = 0) -> dict:
    key_list = jax.random.split(jax.random.key(seed), 3)
    return {
        "lattice_links": draw_lattice_links(jax.random.fold_in(key_list[2], 71), 0),
        "transform": draw_transform(jax.random.fold_in(key_list[2], 71), 0),
    }


OMEGA = 1.7
GUARD = 1e-12

def split_matrix(values):
    lead = values.shape[1:]
    return (values[:9].reshape((3, 3) + lead), values[9:].reshape((3, 3) + lead))

def join_matrix(mat_re, mat_im):
    lead = mat_re.shape[2:]
    return jnp.concatenate([mat_re.reshape((9,) + lead), mat_im.reshape((9,) + lead)], 0)

def product(left_re, left_im, right_re, right_im):
    total_re = None
    total_im = None
    for inner in range(3):
        col_re = left_re[:, inner][:, None]
        col_im = left_im[:, inner][:, None]
        row_re = right_re[inner][None]
        row_im = right_im[inner][None]
        term_re = col_re * row_re - col_im * row_im
        term_im = col_re * row_im + col_im * row_re
        if total_re is None:
            total_re = term_re
            total_im = term_im
        else:
            total_re = total_re + term_re
            total_im = total_im + term_im
    return (total_re, total_im)

def adjoint(mat_re, mat_im):
    return (jnp.swapaxes(mat_re, 0, 1), -jnp.swapaxes(mat_im, 0, 1))

def along_x(values, offset, forward, half_len):
    column = jnp.arange(values.shape[-1], dtype=jnp.int32) % half_len
    if forward:
        stepped = jnp.where(column == half_len - 1, jnp.roll(values, half_len - 1, -1), jnp.roll(values, -1, -1))
        return jnp.where(offset == 0, values, stepped)
    stepped = jnp.where(column == 0, jnp.roll(values, 1 - half_len, -1), jnp.roll(values, 1, -1))
    return jnp.where(offset == 0, stepped, values)

def rotation(mat_re, mat_im, row_one, row_two):
    vec_zero = mat_re[row_one, row_one] + mat_re[row_two, row_two]
    vec_one = -(mat_im[row_one, row_two] + mat_im[row_two, row_one])
    vec_two = mat_re[row_two, row_one] - mat_re[row_one, row_two]
    vec_three = -(mat_im[row_one, row_one] - mat_im[row_two, row_two])
    length = jnp.sqrt(vec_zero * vec_zero + vec_one * vec_one + vec_two * vec_two + vec_three * vec_three)
    step_zero = (1.0 - OMEGA) * length + OMEGA * vec_zero
    step_one = OMEGA * vec_one
    step_two = OMEGA * vec_two
    step_three = OMEGA * vec_three
    divisor = jnp.sqrt(step_zero * step_zero + step_one * step_one + step_two * step_two + step_three * step_three + GUARD)
    return (step_zero / divisor, step_one / divisor, step_two / divisor, step_three / divisor)

def rotate(mat_re, mat_im, quat, row_one, row_two):
    q_zero, q_one, q_two, q_three = quat
    upper_re, upper_im = (mat_re[row_one], mat_im[row_one])
    lower_re, lower_im = (mat_re[row_two], mat_im[row_two])

    def combine(left_pair, right_pair):
        left_re, left_im = (left_pair[0][None], left_pair[1][None])
        right_re, right_im = (right_pair[0][None], right_pair[1][None])
        new_re = left_re * upper_re - left_im * upper_im + right_re * lower_re - right_im * lower_im
        new_im = left_re * upper_im + left_im * upper_re + right_re * lower_im + right_im * lower_re
        return (new_re, new_im)
    top_re, top_im = combine((q_zero, q_three), (q_two, q_one))
    bottom_re, bottom_im = combine((-q_two, q_one), (q_zero, -q_three))
    rows_re = [mat_re[0], mat_re[1], mat_re[2]]
    rows_im = [mat_im[0], mat_im[1], mat_im[2]]
    rows_re[row_one] = top_re
    rows_im[row_one] = top_im
    rows_re[row_two] = bottom_re
    rows_im[row_two] = bottom_im
    return (jnp.stack(rows_re, 0), jnp.stack(rows_im, 0))

def relax(own, own_links, forward, backward):
    gauge_re, gauge_im = split_matrix(own)
    sum_re = None
    sum_im = None
    for direction in range(4):
        link_re, link_im = split_matrix(own_links[direction])
        next_re, next_im = adjoint(forward[direction][0], forward[direction][1])
        ahead_re, ahead_im = product(link_re, link_im, next_re, next_im)
        behind_re, behind_im = adjoint(backward[direction][0], backward[direction][1])
        if sum_re is None:
            sum_re = ahead_re + behind_re
            sum_im = ahead_im + behind_im
        else:
            sum_re = sum_re + ahead_re + behind_re
            sum_im = sum_im + ahead_im + behind_im
    mat_re, mat_im = product(gauge_re, gauge_im, sum_re, sum_im)
    for row_one, row_two in ((0, 1), (0, 2), (1, 2)):
        quat = rotation(mat_re, mat_im, row_one, row_two)
        mat_re, mat_im = rotate(mat_re, mat_im, quat, row_one, row_two)
        gauge_re, gauge_im = rotate(gauge_re, gauge_im, quat, row_one, row_two)
    return (join_matrix(gauge_re, gauge_im), mat_re, mat_im)

def measures(mat_re, mat_im):
    diag_sum = mat_re[0, 0] + mat_re[1, 1] + mat_re[2, 2]
    skew_re = 0.5 * (mat_re - jnp.swapaxes(mat_re, 0, 1))
    skew_im = 0.5 * (mat_im + jnp.swapaxes(mat_im, 0, 1))
    mean_im = (skew_im[0, 0] + skew_im[1, 1] + skew_im[2, 2]) / 3.0
    identity = jnp.eye(3, dtype=jnp.float32).reshape((3, 3) + (1,) * diag_sum.ndim)
    skew_im = skew_im - identity * mean_im[None, None]
    return (jnp.sum(diag_sum), jnp.sum(skew_re * skew_re + skew_im * skew_im))

def neighbour(values, direction, sign, offset, half_len):
    if direction == 0:
        return along_x(values, offset, sign > 0, half_len)
    if direction == 1:
        return jnp.roll(values, -sign * half_len, -1)
    if direction == 2:
        return jnp.roll(values, -sign, -2)
    return jnp.roll(values, -sign, -3)

def reference(lattice_links, transform):
    half_len = NX // 2
    row_len = lattice_links.shape[-1]
    t_index = jnp.arange(NT, dtype=jnp.int32)[:, None, None]
    z_index = jnp.arange(NZ, dtype=jnp.int32)[None, :, None]
    y_index = (jnp.arange(row_len, dtype=jnp.int32) // half_len)[None, None, :]
    parity = t_index + z_index + y_index
    offsets = [parity % 2, (parity + 1) % 2]
    colours = [transform[0], transform[1]]
    func_list = []
    div_list = []
    for sweep in range(ITERS):
        for colour in (0, 1):
            partner = 1 - colour
            offset = offsets[colour]
            part_re, part_im = split_matrix(colours[partner])
            forward = []
            backward = []
            for direction in range(4):
                forward.append((neighbour(part_re, direction, 1, offset, half_len), neighbour(part_im, direction, 1, offset, half_len)))
                link_re, link_im = split_matrix(lattice_links[partner, direction])
                prod_re, prod_im = product(part_re, part_im, link_re, link_im)
                backward.append((neighbour(prod_re, direction, -1, offset, half_len), neighbour(prod_im, direction, -1, offset, half_len)))
            colours[colour], mat_re, mat_im = relax(colours[colour], lattice_links[colour], forward, backward)
        func_sum, div_sum = measures(mat_re, mat_im)
        func_list.append(func_sum)
        div_list.append(div_sum)
    volume = NT * NZ * NY * NX
    sums = jnp.stack([jnp.stack(func_list), jnp.stack(div_list)], 0)
    monitor = jnp.stack([1.0 - sums[0] / (12.0 * volume), sums[1] / (volume / 2.0)], 0)
    return (jnp.stack(colours, 0), monitor)
```

```python
import functools

import jax
import jax.numpy as jnp
from jax import lax
from jax.experimental import pallas as pl
from jax.experimental.pallas import tpu as pltpu
from jax.sharding import PartitionSpec as P

NX = 64
ITERS = 2
OMEGA = 1.7
GUARD = 1e-12
LANES = 128
AXES = ("ta", "gz", "gy")
MESH = pl.DeviceIdType.MESH


def total(terms):
    out = terms[0]
    for term in terms[1:]:
        out = out + term
    return out


def mul(a, b):
    re, im = [], []
    for i in range(3):
        for j in range(3):
            re.append(
                total([a[3 * i + k] * b[3 * k + j] for k in range(3)])
                - total([a[9 + 3 * i + k] * b[9 + 3 * k + j] for k in range(3)])
            )
            im.append(
                total([a[3 * i + k] * b[9 + 3 * k + j] for k in range(3)])
                + total([a[9 + 3 * i + k] * b[3 * k + j] for k in range(3)])
            )
    return re + im


def mul_adj(a, b):
    re, im = [], []
    for i in range(3):
        for j in range(3):
            re.append(
                total([a[3 * i + k] * b[3 * j + k] for k in range(3)])
                + total([a[9 + 3 * i + k] * b[9 + 3 * j + k] for k in range(3)])
            )
            im.append(
                total([a[9 + 3 * i + k] * b[3 * j + k] for k in range(3)])
                - total([a[3 * i + k] * b[9 + 3 * j + k] for k in range(3)])
            )
    return re + im


def add(a, b):
    return [x + y for x, y in zip(a, b)]


def add_adj(a, b):
    out = []
    for i in range(3):
        for j in range(3):
            out.append(a[3 * i + j] + b[3 * j + i])
    for i in range(3):
        for j in range(3):
            out.append(a[9 + 3 * i + j] - b[9 + 3 * j + i])
    return out


def rotation(a, i, j):
    ii, jj, ij, ji = 4 * i, 4 * j, 3 * i + j, 3 * j + i
    v0 = a[ii] + a[jj]
    v1 = -(a[9 + ij] + a[9 + ji])
    v2 = a[ji] - a[ij]
    v3 = a[9 + jj] - a[9 + ii]
    tail = v1 * v1 + v2 * v2 + v3 * v3
    length = jnp.sqrt(v0 * v0 + tail)
    s0 = (1.0 - OMEGA) * length + OMEGA * v0
    inv = lax.rsqrt(s0 * s0 + (OMEGA * OMEGA) * tail + GUARD)
    scaled = OMEGA * inv
    return (s0 * inv, v1 * scaled, v2 * scaled, v3 * scaled)


def rotate(m, q, i, j):
    q0, q1, q2, q3 = q
    out = list(m)
    for k in range(3):
        ur, ui = m[3 * i + k], m[9 + 3 * i + k]
        lr, li = m[3 * j + k], m[9 + 3 * j + k]
        out[3 * i + k] = q0 * ur - q3 * ui + q2 * lr - q1 * li
        out[9 + 3 * i + k] = q0 * ui + q3 * ur + q2 * li + q1 * lr
        out[3 * j + k] = q0 * lr + q3 * li - q2 * ur - q1 * ui
        out[9 + 3 * j + k] = q0 * li - q3 * lr - q2 * ui + q1 * ur
    return out


def third_row(m):
    re, im = list(m[:6]), list(m[6:])
    for k in range(3):
        a, b = (k + 1) % 3, (k + 2) % 3
        re.append(
            m[a] * m[3 + b] - m[6 + a] * m[9 + b] - m[b] * m[3 + a] + m[6 + b] * m[9 + a]
        )
        im.append(
            m[b] * m[9 + a] + m[6 + b] * m[3 + a] - m[a] * m[9 + b] - m[6 + a] * m[3 + b]
        )
    return re + im


def two_rows(m):
    return m[:6] + m[9:15]


PAIRS = ((0, 1), (0, 2), (1, 2))


def kernel(
    sizes,
    links_hbm,
    trans_hbm,
    g,
    mon_out,
    links,
    w,
    py,
    pz,
    tsend,
    trecv,
    halo,
    fsend,
    zsend,
    zrecv,
    ysend,
    yrecv,
    mon,
    plane,
    load_sem,
    t_send_sem,
    t_recv_sem,
    send_sem,
    recv_sem,
    red_send,
    red_recv,
):
    slices, depth, row_len = g.shape[2:]
    nh = row_len // LANES
    half = NX // 2
    strips = LANES // half
    groups = ysend.shape[3]
    last = slices - 1
    steps = 2 * ITERS
    me = {a: lax.axis_index(a) for a in AXES}

    def peer(axis, d):
        n = sizes[axis]
        return {axis: lax.rem(me[axis] + d + n, n)}

    loads = [
        pltpu.make_async_copy(trans_hbm.at[1], g.at[1], load_sem.at[0]),
        pltpu.make_async_copy(links_hbm.at[1], links.at[1], load_sem.at[1]),
        pltpu.make_async_copy(trans_hbm.at[0], g.at[0], load_sem.at[2]),
        pltpu.make_async_copy(links_hbm.at[0], links.at[0], load_sem.at[3]),
    ]
    for copy in loads:
        copy.start()
    barrier = pltpu.get_barrier_semaphore()
    near = [(a, d) for a in AXES for d in sorted({1, sizes[a] - 1})]
    for axis, d in near:
        pl.semaphore_signal(barrier, inc=1, device_id=peer(axis, d), device_id_type=MESH)
    mon[...] = jnp.zeros_like(mon)
    pl.semaphore_wait(barrier, len(near))

    row = lax.broadcasted_iota(jnp.int32, (depth, LANES), 0)
    lane = lax.broadcasted_iota(jnp.int32, (depth, LANES), 1)
    column = lane % half
    strip = lane // half

    def piece(h):
        return pl.ds(h * LANES if isinstance(h, int) else pl.multiple_of(h * LANES, LANES), LANES)

    def load(ref, *index):
        t, h = index[-2:]
        return [ref[index[:-2] + (comp, t, slice(None), piece(h))] for comp in range(18)]

    def store(ref, values, *index):
        t, h = index[-2:]
        for comp in range(18):
            ref[index[:-2] + (comp, t, slice(None), piece(h))] = values[comp]

    def remote(src, dst, k, number, axis, d):
        return pltpu.make_async_remote_copy(
            src_ref=src,
            dst_ref=dst,
            send_sem=send_sem.at[k, number],
            recv_sem=recv_sem.at[k, number],
            device_id=peer(axis, d),
            device_id_type=MESH,
        )

    def t_copy(slot, way, h):
        return pltpu.make_async_remote_copy(
            src_ref=tsend.at[slot, way, :, :, piece(h)],
            dst_ref=trecv.at[slot, way, :, :, piece(h)],
            send_sem=t_send_sem.at[slot, way, h],
            recv_sem=t_recv_sem.at[slot, way, h],
            device_id=peer("ta", 1 if way else -1),
            device_id_type=MESH,
        )

    def full_copy(way, h):
        return pltpu.make_async_remote_copy(
            src_ref=fsend.at[way, :, :, piece(h)],
            dst_ref=halo.at[0, way, :, :, piece(h)],
            send_sem=t_send_sem.at[steps + 1, way, h],
            recv_sem=t_recv_sem.at[steps + 1, way, h],
            device_id=peer("ta", 1 if way else -1),
            device_id_type=MESH,
        )

    def send_full(way, h):
        values = load(g, 0, last if way else 0, h)
        if way:
            values = mul(values, load(links, 0, 3, last, h))
        put(fsend, (way,), h, values)
        full_copy(way, h).start()

    def side(k):
        return [
            remote(ysend.at[k, 0], yrecv.at[k, 0], k, 2, "gy", -1),
            remote(ysend.at[k, 1], yrecv.at[k, 1], k, 3, "gy", 1),
            remote(zsend.at[k, 0], zrecv.at[k, 0], k, 0, "gz", -1),
            remote(zsend.at[k, 1], zrecv.at[k, 1], k, 1, "gz", 1),
        ]

    def put(ref, index, h, values):
        for number, value in enumerate(values):
            ref[index + (number, slice(None), piece(h))] = value

    def get(ref, index, h, count):
        return [ref[index + (number, slice(None), piece(h))] for number in range(count)]

    def send_given(slot, colour, h):
        put(tsend, (slot, 0), h, two_rows(load(g, colour, 0, h)))
        t_copy(slot, 0, h).start()
        prod = mul(load(g, colour, last, h), load(links, colour, 3, last, h))
        put(tsend, (slot, 1), h, two_rows(prod))
        t_copy(slot, 1, h).start()

    def take_given(slot, colour, way, h):
        t_copy(slot, way, h).wait_recv()
        put(halo, (colour, way), h, third_row(get(trecv, (slot, way), h, 12)))

    def take_turned(slot, colour, way, h):
        t_copy(slot, way, h).wait_recv()
        q = get(trecv, (slot, way), h, 12)
        m = get(halo, (colour, way), h, 18)
        for number, (i, j) in enumerate(PAIRS):
            m = rotate(m, q[4 * number : 4 * number + 4], i, j)
        put(halo, (colour, way), h, m)

    def pack(values, ref, k, way, t):
        for group in range(groups):
            tile = None
            for j in range(strips):
                comp = group * strips + j
                if comp >= 18:
                    continue
                turn = (half * (j + way)) % LANES
                moved = pltpu.roll(values[comp], turn, 1) if turn else values[comp]
                tile = moved if tile is None else jnp.where(strip == j, moved, tile)
            ref[k, way, t, group] = tile

    def unpack(ref, k, way, t):
        out = []
        for comp in range(18):
            group, j = comp // strips, comp % strips
            tile = ref[k, way, t, group]
            turn = (LANES - half - half * j if way == 0 else LANES - half * j) % LANES
            out.append(pltpu.roll(tile, turn, 1) if turn else tile)
        return out

    def products(k, p, t, h, other):
        prod_y = mul(other, load(links, p, 1, t, h))
        store(py, prod_y, t, h)
        if h == 0:
            pack(other, ysend, k, 0, t)
        if h == nh - 1:
            pack(prod_y, ysend, k, 1, t)
        prod_z = mul(other, load(links, p, 2, t, h))
        store(pz, prod_z, t, h)
        for comp in range(18):
            zsend[k, 0, t, comp : comp + 1, piece(h)] = other[comp][0:1]
            zsend[k, 1, t, comp : comp + 1, piece(h)] = prod_z[comp][depth - 1 : depth]

    def half_sweep(n, c):
        p = 1 - c
        k = 2 * n + c
        sides = side(k)
        if c == 0:
            @pl.when(n == 0)
            def _():
                loads[2].wait()
                loads[3].wait()

        def along_x(t, _):
            offset = (row + strip + (t + c)) % 2
            for h in range(nh):
                other = load(g, p, t, h)
                ahead = []
                for v in other:
                    stepped = jnp.where(
                        column == half - 1, pltpu.roll(v, half - 1, 1), pltpu.roll(v, LANES - 1, 1)
                    )
                    ahead.append(jnp.where(offset == 0, v, stepped))
                acc = mul_adj(load(links, c, 0, t, h), ahead)
                behind = []
                for v in mul(other, load(links, p, 0, t, h)):
                    stepped = jnp.where(
                        column == 0, pltpu.roll(v, LANES - half + 1, 1), pltpu.roll(v, 1, 1)
                    )
                    behind.append(jnp.where(offset == 0, stepped, v))
                store(w, add_adj(acc, behind), t, h)
            return 0

        lax.fori_loop(0, slices, along_x, 0)

        def inner_t(h, _):
            for t in range(last):
                near = mul_adj(load(links, c, 3, t, h), load(g, p, t + 1, h))
                store(w, add(load(w, t, h), near), t, h)
                back = mul(load(g, p, t, h), load(links, p, 3, t, h))
                store(w, add_adj(load(w, t + 1, h), back), t + 1, h)
            return 0

        lax.fori_loop(0, nh, inner_t, 0)
        for copy in sides:
            copy.wait_recv()

        def along_yz(t, _):
            for h in range(nh):
                acc = load(w, t, h)
                behind, ahead = [], []
                prod_z = load(pz, t, h)
                other = load(g, p, t, h)
                for comp in range(18):
                    edge = zrecv[k, 0, t, comp : comp + 1, piece(h)]
                    edge = jnp.broadcast_to(edge, (depth, LANES))
                    moved = pltpu.roll(other[comp], depth - 1, 0)
                    ahead.append(jnp.where(row == depth - 1, edge, moved))
                    edge = zrecv[k, 1, t, comp : comp + 1, piece(h)]
                    edge = jnp.broadcast_to(edge, (depth, LANES))
                    behind.append(jnp.where(row == 0, edge, pltpu.roll(prod_z[comp], 1, 0)))
                acc = add_adj(acc, behind)
                acc = add(acc, mul_adj(load(links, c, 2, t, h), ahead))
                if h == nh - 1:
                    edge = unpack(yrecv, k, 0, t)
                else:
                    edge = [pltpu.roll(v, LANES - half, 1) for v in load(g, p, t, h + 1)]
                ahead = [
                    jnp.where(strip == strips - 1, e, pltpu.roll(v, LANES - half, 1))
                    for e, v in zip(edge, other)
                ]
                acc = add(acc, mul_adj(load(links, c, 1, t, h), ahead))
                if h == 0:
                    edge = unpack(yrecv, k, 1, t)
                else:
                    edge = [pltpu.roll(v, half, 1) for v in load(py, t, h - 1)]
                behind = [
                    jnp.where(strip == 0, e, pltpu.roll(v, half, 1))
                    for e, v in zip(edge, load(py, t, h))
                ]
                store(w, add_adj(acc, behind), t, h)
            return 0

        lax.fori_loop(0, slices, along_yz, 0)

        def finish(t, h, acc):
            own = load(g, c, t, h)
            a = mul(own, acc)
            turns = []
            for i, j in PAIRS:
                q = rotation(a, i, j)
                turns.extend(q)
                a = rotate(a, q, i, j)
                own = rotate(own, q, i, j)
            if t == last:
                put(tsend, (k + 1, 1), h, turns)
            if t == 0:
                put(tsend, (k + 1, 0), h, turns)
            store(g, own, c, t, h)
            if c == 1:
                func = a[0] + a[4] + a[8]
                mean = (a[9] + a[13] + a[17]) * (1.0 / 3.0)
                div = None
                for i in range(3):
                    d = a[9 + 4 * i] - mean
                    div = d * d if div is None else div + d * d
                for i, j in ((0, 1), (0, 2), (1, 2)):
                    d = a[3 * i + j] - a[3 * j + i]
                    e = a[9 + 3 * i + j] + a[9 + 3 * j + i]
                    div = div + 0.5 * (d * d + e * e)
                mon[n, 0] += func
                mon[n, 1] += div

        def onward(action):
            if c == 0:
                action()
            else:
                pl.when(k + 1 < steps)(action)

        def pass_on(way, h):
            if c == 0:
                @pl.when(n == 0)
                def _():
                    send_full(way, h)

                @pl.when(n > 0)
                def _():
                    t_copy(k + 1, way, h).start()
            else:
                @pl.when(k + 1 < steps)
                def _():
                    t_copy(k + 1, way, h).start()

        def take(way, h):
            if c == 1:
                @pl.when(n == 0)
                def _():
                    full_copy(way, h).wait_recv()

                @pl.when(n > 0)
                def _():
                    take_turned(k, p, way, h)
            else:
                @pl.when(n == 0)
                def _():
                    take_given(k, p, way, h)

                @pl.when(n > 0)
                def _():
                    take_turned(k, p, way, h)

        for h in range(nh):
            take(0, h)
            edge = get(halo, (p, 0), h, 18)
            finish(last, h, add(load(w, last, h), mul_adj(load(links, c, 3, last, h), edge)))
            pass_on(1, h)
            for t in range(1, last):
                finish(t, h, load(w, t, h))
            take(1, h)
            edge = get(halo, (p, 1), h, 18)
            finish(0, h, add_adj(load(w, 0, h), edge))

            pass_on(0, h)

            def after():
                for t in range(slices):
                    products(k + 1, c, t, h, load(g, c, t, h))
                follow = side(k + 1)
                if h == 0:
                    follow[0].start()
                if h == nh - 1:
                    for copy in follow[1:]:
                        copy.start()

            onward(after)

    loads[0].wait()
    loads[1].wait()
    for h in range(nh):
        send_given(0, 1, h)
    for h in range(nh):
        for t in range(slices):
            products(0, 1, t, h, load(g, 1, t, h))
    for copy in side(0):
        copy.start()

    def iteration(n, _):
        half_sweep(n, 0)
        half_sweep(n, 1)
        return 0

    lax.fori_loop(0, ITERS, iteration, 0)

    spot = lax.broadcasted_iota(jnp.int32, (1, LANES), 1)
    sums = jnp.zeros((1, LANES), jnp.float32)
    for n in range(ITERS):
        for part in range(2):
            value = jnp.sum(jnp.sum(mon[n, part], axis=0, keepdims=True), axis=1, keepdims=True)
            sums = jnp.where(spot == 2 * n + part, value, sums)

    lines = plane.shape[0]
    here = (me["ta"] * sizes["gz"] + me["gz"]) * sizes["gy"] + me["gy"]
    plane[here] = sums
    offsets = [
        (i, j, k)
        for i in range(sizes["ta"])
        for j in range(sizes["gz"])
        for k in range(sizes["gy"])
        if i or j or k
    ]

    def to_other(i, j, k):
        return pltpu.make_async_remote_copy(
            src_ref=plane.at[here],
            dst_ref=plane.at[here],
            send_sem=red_send,
            recv_sem=red_recv,
            device_id=peer("ta", i) | peer("gz", j) | peer("gy", k),
            device_id_type=MESH,
        )

    for offset in reversed(offsets):
        to_other(*offset).start()
    width = sizes["gz"] * sizes["gy"]
    arrivals = pltpu.make_async_remote_copy(
        src_ref=plane.at[pl.ds(0, lines - 1)],
        dst_ref=plane.at[pl.ds(0, lines - 1)],
        send_sem=red_send,
        recv_sem=red_recv,
        device_id=peer("ta", 1),
        device_id_type=MESH,
    )
    arrivals.wait_recv()
    sums = total([plane[number] for number in range(lines)])
    sites = slices * depth * row_len * sizes["ta"] * width
    for n in range(ITERS):
        mon_out[0, n] = 1.0 - sums[0, 2 * n] / (24.0 * sites)
        mon_out[1, n] = sums[0, 2 * n + 1] / float(sites)
    arrivals.wait_send()
    for h in range(nh):
        for way in range(2):
            full_copy(way, h).wait_send()
            for slot in range(steps):
                if slot != 1:
                    t_copy(slot, way, h).wait_send()
    for k in range(steps):
        for copy in side(k):
            copy.wait_send()


def shards(sizes, lattice_links, transform):
    slices, depth, row_len = transform.shape[2:]
    nh = row_len // LANES
    strips = LANES // (NX // 2)
    groups = -(-18 // strips)
    steps = 2 * ITERS
    face = (18, slices, depth, row_len)
    assert depth == 8 and slices > 1 and row_len % LANES == 0
    f32 = jnp.float32
    width = sizes["gz"] * sizes["gy"]
    lines = width * sizes["ta"]
    g, mon = pl.pallas_call(
        functools.partial(kernel, sizes),
        out_shape=(
            pltpu.VMEM(transform.shape, f32),
            pltpu.SMEM((2, ITERS), f32),
        ),
        in_specs=[pl.BlockSpec(memory_space=pltpu.HBM)] * 2,
        out_specs=(
            pl.BlockSpec(memory_space=pltpu.VMEM),
            pl.BlockSpec(memory_space=pltpu.SMEM),
        ),
        scratch_shapes=[
            pltpu.VMEM(lattice_links.shape, f32),
            pltpu.VMEM(face, f32),
            pltpu.VMEM(face, f32),
            pltpu.VMEM(face, f32),
            pltpu.VMEM((steps + 2, 2, 12, depth, row_len), f32),
            pltpu.VMEM((steps + 2, 2, 12, depth, row_len), f32),
            pltpu.VMEM((2, 2, 18, depth, row_len), f32),
            pltpu.VMEM((2, 18, depth, row_len), f32),
            pltpu.VMEM((steps, 2, slices, 18, row_len), f32),
            pltpu.VMEM((steps, 2, slices, 18, row_len), f32),
            pltpu.VMEM((steps, 2, slices, groups, depth, LANES), f32),
            pltpu.VMEM((steps, 2, slices, groups, depth, LANES), f32),
            pltpu.VMEM((ITERS, 2, depth, LANES), f32),
            pltpu.VMEM((lines, 1, LANES), f32),
            pltpu.SemaphoreType.DMA((4,)),
            pltpu.SemaphoreType.DMA((steps + 2, 2, nh)),
            pltpu.SemaphoreType.DMA((steps + 2, 2, nh)),
            pltpu.SemaphoreType.DMA((steps, 4)),
            pltpu.SemaphoreType.DMA((steps, 4)),
            pltpu.SemaphoreType.DMA,
            pltpu.SemaphoreType.DMA,
        ],
        compiler_params=pltpu.CompilerParams(
            collective_id=0, has_side_effects=True, vmem_limit_bytes=67043328 - 900000 // 4096 * 4096
        ),
    )(lattice_links, transform)

    def finish(g_ref, mon_ref, out_ref, mon_out, sem, sem2):
        copy = pltpu.make_async_copy(g_ref, out_ref, sem)
        copy.start()
        small = pltpu.make_async_copy(mon_ref, mon_out, sem2)
        small.start()
        copy.wait()
        small.wait()

    return pl.pallas_call(
        finish,
        out_shape=(
            jax.ShapeDtypeStruct(transform.shape, f32),
            jax.ShapeDtypeStruct((2, ITERS), f32),
        ),
        in_specs=[pl.BlockSpec(memory_space=pltpu.VMEM), pl.BlockSpec(memory_space=pltpu.SMEM)],
        out_specs=(pl.BlockSpec(memory_space=pltpu.HBM), pl.BlockSpec(memory_space=pltpu.HBM)),
        scratch_shapes=[pltpu.SemaphoreType.DMA,pltpu.SemaphoreType.DMA],
        compiler_params=pltpu.CompilerParams(vmem_limit_bytes=1 << 20),
    )(g, mon)


def solution(mesh):
    sizes = {axis: mesh.shape[axis] for axis in AXES}
    return jax.shard_map(
        functools.partial(shards, sizes),
        mesh=mesh,
        in_specs=(P(None, None, None, "ta", "gz", "gy"), P(None, None, "ta", "gz", "gy")),
        out_specs=(P(None, None, "ta", "gz", "gy"), P()),
        check_vma=False,
    )
```

```python
import functools

import jax
import jax.numpy as jnp
from jax import lax
from jax.experimental import pallas as pl
from jax.experimental.pallas import tpu as pltpu
from jax.sharding import PartitionSpec as P

NX = 64
ITERS = 2
OMEGA = 1.7
GUARD = 1e-12
FLOOR = 1e-20
FAR = 1e15
LANES = 128
AXES = ("ta", "gz", "gy")
MESH = pl.DeviceIdType.MESH


def total(terms):
    out = terms[0]
    for term in terms[1:]:
        out = out + term
    return out


def mul(a, b):
    re, im = [], []
    for i in range(3):
        for j in range(3):
            re.append(
                total([a[3 * i + k] * b[3 * k + j] for k in range(3)])
                - total([a[9 + 3 * i + k] * b[9 + 3 * k + j] for k in range(3)])
            )
            im.append(
                total([a[3 * i + k] * b[9 + 3 * k + j] for k in range(3)])
                + total([a[9 + 3 * i + k] * b[3 * k + j] for k in range(3)])
            )
    return re + im


def mul_adj(a, b):
    re, im = [], []
    for i in range(3):
        for j in range(3):
            re.append(
                total([a[3 * i + k] * b[3 * j + k] for k in range(3)])
                + total([a[9 + 3 * i + k] * b[9 + 3 * j + k] for k in range(3)])
            )
            im.append(
                total([a[9 + 3 * i + k] * b[3 * j + k] for k in range(3)])
                - total([a[3 * i + k] * b[9 + 3 * j + k] for k in range(3)])
            )
    return re + im


def add(a, b):
    return [x + y for x, y in zip(a, b)]


def add_adj(a, b):
    out = []
    for i in range(3):
        for j in range(3):
            out.append(a[3 * i + j] + b[3 * j + i])
    for i in range(3):
        for j in range(3):
            out.append(a[9 + 3 * i + j] - b[9 + 3 * j + i])
    return out


def rotation(a, i, j):
    ii, jj, ij, ji = 4 * i, 4 * j, 3 * i + j, 3 * j + i
    v0 = a[ii] + a[jj]
    v1 = -(a[9 + ij] + a[9 + ji])
    v2 = a[ji] - a[ij]
    v3 = a[9 + jj] - a[9 + ii]
    tail = v1 * v1 + v2 * v2 + v3 * v3
    length = jnp.sqrt(v0 * v0 + tail)
    s0 = (1.0 - OMEGA) * length + OMEGA * v0
    inv = lax.rsqrt(s0 * s0 + (OMEGA * OMEGA) * tail + GUARD)
    scaled = OMEGA * inv
    return (s0 * inv, v1 * scaled, v2 * scaled, v3 * scaled)


def rotate(m, q, i, j):
    q0, q1, q2, q3 = q
    out = list(m)
    for k in range(3):
        ur, ui = m[3 * i + k], m[9 + 3 * i + k]
        lr, li = m[3 * j + k], m[9 + 3 * j + k]
        out[3 * i + k] = q0 * ur - q3 * ui + q2 * lr - q1 * li
        out[9 + 3 * i + k] = q0 * ui + q3 * ur + q2 * li + q1 * lr
        out[3 * j + k] = q0 * lr + q3 * li - q2 * ur - q1 * ui
        out[9 + 3 * j + k] = q0 * li - q3 * lr - q2 * ui + q1 * ur
    return out


def third_row(m):
    re, im = list(m[:6]), list(m[6:])
    for k in range(3):
        a, b = (k + 1) % 3, (k + 2) % 3
        re.append(
            m[a] * m[3 + b] - m[6 + a] * m[9 + b] - m[b] * m[3 + a] + m[6 + b] * m[9 + a]
        )
        im.append(
            m[b] * m[9 + a] + m[6 + b] * m[3 + a] - m[a] * m[9 + b] - m[6 + a] * m[3 + b]
        )
    return re + im


def to_flat(x, v):
    square = total([c * c for c in v])
    scale = jnp.where(x >= 0.0, 1.0 + x, square / (1.0 + jnp.abs(x)))
    pole = scale < FLOOR
    inv = 1.0 / jnp.where(pole, 1.0, scale)
    flat = [c * inv for c in v]
    return [jnp.where(pole, FAR, flat[0])] + [jnp.where(pole, 0.0, c) for c in flat[1:]]


def from_flat(flat):
    scale = 2.0 / (1.0 + total([c * c for c in flat]))
    return [scale - 1.0] + [c * scale for c in flat]


def cmul(a, b):
    return (a[0] * b[0] - a[1] * b[1], a[0] * b[1] + a[1] * b[0])


def cmul_conj(a, b):
    return (a[0] * b[0] + a[1] * b[1], a[1] * b[0] - a[0] * b[1])


def first_row(flat):
    r0, i0, r1, i1, r2, i2 = from_flat(flat)
    square = r0 * r0 + i0 * i0 + r1 * r1 + i1 * i1
    small = square < FLOOR
    inv = lax.rsqrt(jnp.where(small, 1.0, square))
    c0 = (jnp.where(small, 1.0, r0 * inv), jnp.where(small, 0.0, i0 * inv))
    c1 = (jnp.where(small, 0.0, r1 * inv), jnp.where(small, 0.0, i1 * inv))
    norm = jnp.where(small, 0.0, square * inv)
    return [r0, r1, r2], [i0, i1, i2], c0, c1, norm


def encode(m):
    flat = to_flat(m[0], [m[9], m[1], m[10], m[2], m[11]])
    re, im, c0, c1, norm = first_row(flat)
    a2 = (re[2], im[2])
    b0, b1, b2 = [(m[3 + k], m[12 + k]) for k in range(3)]
    x, y = cmul(b1, c0), cmul(b0, c1)
    u, v = cmul_conj(b0, c0), cmul_conj(b1, c1)
    w = cmul(a2, (u[0] + v[0], u[1] + v[1]))
    return flat + to_flat(
        x[0] - y[0], [x[1] - y[1], norm * b2[0] - w[0], norm * b2[1] - w[1]]
    )


def decode(values):
    re, im, c0, c1, norm = first_row(values[:5])
    p0, p1, r0, r1 = from_flat(values[5:])
    p, r = (p0, p1), (r0, r1)
    turn = cmul_conj(r, (re[2], im[2]))
    x, y = cmul_conj(p, c1), cmul(turn, c0)
    u, v = cmul_conj(p, c0), cmul(turn, c1)
    return third_row(
        re + [-x[0] - y[0], u[0] - v[0], norm * r0]
        + im + [-x[1] - y[1], u[1] - v[1], norm * r1]
    )


PAIRS = ((0, 1), (0, 2), (1, 2))


def kernel(
    sizes,
    links_hbm,
    trans_hbm,
    g,
    mon_out,
    links,
    w,
    cb,
    py,
    pz,
    tsend,
    trecv,
    halo,
    esend,
    erecv,
    zsend,
    zrecv,
    ysend,
    yrecv,
    mon,
    plane,
    load_sem,
    t_send_sem,
    t_recv_sem,
    first_send_sem,
    first_recv_sem,
    side_send_sem,
    side_recv_sem,
    red_send,
    red_recv,
):
    slices, depth, row_len = g.shape[2:]
    nh = row_len // LANES
    half = NX // 2
    strips = LANES // half
    groups = ysend.shape[3]
    last = slices - 1
    steps = 2 * ITERS
    me = {a: lax.axis_index(a) for a in AXES}

    def peer(axis, d):
        n = sizes[axis]
        return {axis: lax.rem(me[axis] + d + n, n)}

    loads = [
        pltpu.make_async_copy(src, dst, load_sem.at[number])
        for number, (src, dst) in enumerate(
            [
                (trans_hbm.at[1], g.at[1]),
                (links_hbm.at[1, 3], links.at[1, 3]),
                (links_hbm.at[1, pl.ds(1, 2)], links.at[1, pl.ds(1, 2)]),
                (trans_hbm.at[0], g.at[0]),
                (links_hbm.at[0, 3], links.at[0, 3]),
                (links_hbm.at[1, 0], links.at[1, 0]),
                (links_hbm.at[0, pl.ds(0, 3)], links.at[0, pl.ds(0, 3)]),
            ]
        )
    ]
    for copy in loads:
        copy.start()
    barrier = pltpu.get_barrier_semaphore()
    near = [(a, d) for a in AXES for d in sorted({1, sizes[a] - 1})]
    for axis, d in near:
        pl.semaphore_signal(barrier, inc=1, device_id=peer(axis, d), device_id_type=MESH)
    mon[...] = jnp.zeros_like(mon)
    pl.semaphore_wait(barrier, len(near))

    row = lax.broadcasted_iota(jnp.int32, (depth, LANES), 0)
    lane = lax.broadcasted_iota(jnp.int32, (depth, LANES), 1)
    column = lane % half
    strip = lane // half
    flip = (me["ta"] + 1) // sizes["ta"]

    def piece(h):
        return pl.ds(h * LANES if isinstance(h, int) else pl.multiple_of(h * LANES, LANES), LANES)

    def load(ref, *index):
        t, h = index[-2:]
        return [ref[index[:-2] + (comp, t, slice(None), piece(h))] for comp in range(18)]

    def store(ref, values, *index):
        t, h = index[-2:]
        for comp in range(18):
            ref[index[:-2] + (comp, t, slice(None), piece(h))] = values[comp]

    def put(ref, index, h, values):
        for number, value in enumerate(values):
            ref[index + (number, slice(None), piece(h))] = value

    def get(ref, index, h, count):
        return [ref[index + (number, slice(None), piece(h))] for number in range(count)]

    def along_t(way):
        return {"ta": lax.rem(me["ta"] + 2 * way - 1 + sizes["ta"], sizes["ta"])}

    def t_copy(slot, way, h):
        return pltpu.make_async_remote_copy(
            src_ref=tsend.at[slot, way, :, :, piece(h)],
            dst_ref=trecv.at[slot, way, :, :, piece(h)],
            send_sem=t_send_sem.at[slot, way, h],
            recv_sem=t_recv_sem.at[slot, way, h],
            device_id=along_t(way),
            device_id_type=MESH,
        )

    def first_copy(colour, way, h):
        return pltpu.make_async_remote_copy(
            src_ref=esend.at[colour, way, :, :, piece(h)],
            dst_ref=erecv.at[colour, way, :, :, piece(h)],
            send_sem=first_send_sem.at[colour, way, h],
            recv_sem=first_recv_sem.at[colour, way, h],
            device_id=along_t(way),
            device_id_type=MESH,
        )

    def send_first(colour, way, h):
        values = load(g, colour, last if way else 0, h)
        if way:
            values = mul(values, load(links, colour, 3, last, h))
        put(esend, (colour, way), h, encode(values))
        first_copy(colour, way, h).start()

    def take_first(colour, way, h):
        first_copy(colour, way, h).wait_recv()
        m = decode(get(erecv, (colour, way), h, 8))
        put(halo, (colour, way), h, m)
        return m

    def side(k, t):
        ends = [(zsend, zrecv, "gz"), (ysend, yrecv, "gy")]
        return [
            pltpu.make_async_remote_copy(
                src_ref=src.at[k, way, t],
                dst_ref=dst.at[k, way, t],
                send_sem=side_send_sem.at[k, 2 * number + way, t],
                recv_sem=side_recv_sem.at[k, 2 * number + way, t],
                device_id=peer(axis, 1 if way else -1),
                device_id_type=MESH,
            )
            for number, (src, dst, axis) in enumerate(ends)
            for way in range(2)
        ]

    def pack(values, ref, k, way, t):
        for group in range(groups):
            tile = None
            for j in range(strips):
                comp = group * strips + j
                if comp >= 18:
                    continue
                turn = (half * (j + way)) % LANES
                moved = pltpu.roll(values[comp], turn, 1) if turn else values[comp]
                tile = moved if tile is None else jnp.where(strip == j, moved, tile)
            ref[k, way, t, group] = tile

    def unpack(ref, k, way, t):
        out = []
        for comp in range(18):
            group, j = comp // strips, comp % strips
            tile = ref[k, way, t, group]
            turn = (LANES - half - half * j if way == 0 else LANES - half * j) % LANES
            out.append(pltpu.roll(tile, turn, 1) if turn else tile)
        return out

    def products(k, p, t, h, other):
        prod_y = mul(other, load(links, p, 1, t, h))
        store(py, prod_y, t, h)
        if h == 0:
            pack(other, ysend, k, 0, t)
        if h == nh - 1:
            pack(prod_y, ysend, k, 1, t)
        prod_z = mul(other, load(links, p, 2, t, h))
        store(pz, prod_z, t, h)
        for comp in range(18):
            zsend[k, 0, t, comp : comp + 1, piece(h)] = other[comp][0:1]
            zsend[k, 1, t, comp : comp + 1, piece(h)] = prod_z[comp][depth - 1 : depth]

    def turn_own(k, c, t, way, h):
        q = get(tsend, (k, way), h, 12)
        own = load(g, c, t, h)
        for number, (i, j) in enumerate(PAIRS):
            own = rotate(own, q[4 * number : 4 * number + 4], i, j)
        store(g, own, c, t, h)
        return own

    def half_sweep(n, c):
        p = 1 - c
        k = 2 * n + c
        if c == 0:
            @pl.when(n == 0)
            def _():
                for copy in loads[5:]:
                    copy.wait()

        def inside(h, _):
            for t in range(slices):
                offset = (row + strip + (t + c)) % 2
                other = load(g, p, t, h)
                ahead = []
                for v in other:
                    stepped = jnp.where(
                        column == half - 1, pltpu.roll(v, half - 1, 1), pltpu.roll(v, LANES - 1, 1)
                    )
                    ahead.append(jnp.where(offset == 0, v, stepped))
                acc = mul_adj(load(links, c, 0, t, h), ahead)
                behind = []
                for v in mul(other, load(links, p, 0, t, h)):
                    stepped = jnp.where(
                        column == 0, pltpu.roll(v, LANES - half + 1, 1), pltpu.roll(v, 1, 1)
                    )
                    behind.append(jnp.where(offset == 0, stepped, v))
                acc = add_adj(acc, behind)
                if t < last:
                    acc = add(acc, mul_adj(load(links, c, 3, t, h), load(g, p, t + 1, h)))
                if t > 0:
                    acc = add_adj(acc, mul(load(g, p, t - 1, h), load(links, p, 3, t - 1, h)))
                store(w, acc, t, h)

            def outer():
                return (
                    mul(load(g, c, last, h), load(links, c, 3, last, h)),
                    load(g, c, 0, h),
                )

            def turned_halo(way):
                m = get(halo, (p, way), h, 18)
                q = get(trecv, (k - 3, way), h, 12)
                for number, (i, j) in enumerate(PAIRS):
                    m = rotate(m, q[4 * number : 4 * number + 4], i, j)
                put(halo, (p, way), h, m)
                return m

            def prepare(*halos):
                for way, values in enumerate(outer()):
                    if halos:
                        values = mul_adj(halos[0](way), values)
                    put(cb, (way,), h, values)

            if c == 0:
                pl.when(n == 0)(lambda: prepare())
                pl.when(n == 1)(lambda: prepare(lambda way: get(halo, (p, way), h, 18)))
                if ITERS > 2:
                    pl.when(n > 1)(lambda: prepare(turned_halo))
            else:
                pl.when(n == 0)(lambda: prepare(lambda way: take_first(p, way, h)))
                pl.when(n > 0)(lambda: prepare(turned_halo))
            return 0

        lax.fori_loop(0, nh, inside, 0)

        def along_yz(t, h):
            acc = load(w, t, h)
            behind, ahead = [], []
            prod_z = load(pz, t, h)
            other = load(g, p, t, h)
            for comp in range(18):
                edge = zrecv[k, 0, t, comp : comp + 1, piece(h)]
                edge = jnp.broadcast_to(edge, (depth, LANES))
                moved = pltpu.roll(other[comp], depth - 1, 0)
                ahead.append(jnp.where(row == depth - 1, edge, moved))
                edge = zrecv[k, 1, t, comp : comp + 1, piece(h)]
                edge = jnp.broadcast_to(edge, (depth, LANES))
                behind.append(jnp.where(row == 0, edge, pltpu.roll(prod_z[comp], 1, 0)))
            acc = add_adj(acc, behind)
            acc = add(acc, mul_adj(load(links, c, 2, t, h), ahead))
            if h == nh - 1:
                edge = unpack(yrecv, k, 0, t)
            else:
                edge = [pltpu.roll(v, LANES - half, 1) for v in load(g, p, t, h + 1)]
            ahead = [
                jnp.where(strip == strips - 1, e, pltpu.roll(v, LANES - half, 1))
                for e, v in zip(edge, other)
            ]
            acc = add(acc, mul_adj(load(links, c, 1, t, h), ahead))
            if h == 0:
                edge = unpack(yrecv, k, 1, t)
            else:
                edge = [pltpu.roll(v, half, 1) for v in load(py, t, h - 1)]
            behind = [
                jnp.where(strip == 0, e, pltpu.roll(v, half, 1))
                for e, v in zip(edge, load(py, t, h))
            ]
            acc = add_adj(acc, behind)
            store(w, mul(load(g, c, t, h), acc), t, h)

        def take(way, h):
            def turn():
                t_copy(k - 1, way, h).wait_recv()
                q = get(trecv, (k - 1, way), h, 12)
                m = get(cb, (way,), h, 18)
                for number, (i, j) in enumerate(PAIRS):
                    m = rotate(m, q[4 * number : 4 * number + 4], i, j)
                put(cb, (way,), h, m)

            if c == 1:
                turn()
                return

            @pl.when(n == 0)
            def _():
                put(cb, (way,), h, mul_adj(take_first(p, way, h), get(cb, (way,), h, 18)))

            pl.when(n > 0)(turn)

        def monitor(a):
            func = a[0] + a[4] + a[8]
            mean = (a[9] + a[13] + a[17]) * (1.0 / 3.0)
            div = None
            for i in range(3):
                d = a[9 + 4 * i] - mean
                div = d * d if div is None else div + d * d
            for i, j in PAIRS:
                d = a[3 * i + j] - a[3 * j + i]
                e = a[9 + 3 * i + j] + a[9 + 3 * j + i]
                div = div + 0.5 * (d * d + e * e)
            mon[n, 0] += func
            mon[n, 1] += div

        def slab(number, _):
            back = (number + flip) % 2
            ahead = 1 - back
            t = ahead * last
            for copy in side(k, t):
                copy.wait_recv()
            for h in range(nh):
                along_yz(t, h)
            for h in range(nh):
                take(back, h)
                a = add_adj(load(w, t, h), get(cb, (back,), h, 18))
                turns = []
                for i, j in PAIRS:
                    q = rotation(a, i, j)
                    turns.extend(q)
                    a = rotate(a, q, i, j)
                put(tsend, (k, ahead), h, turns)

                if c == 0:
                    t_copy(k, ahead, h).start()
                    products(k + 1, c, t, h, turn_own(k, c, t, ahead, h))
                else:
                    @pl.when(k + 1 < steps)
                    def _():
                        t_copy(k, ahead, h).start()

                    monitor(a)

                    @pl.when(k + 1 < steps)
                    def _():
                        products(k + 1, c, t, h, turn_own(k, c, t, ahead, h))

            def follow():
                for copy in side(k + 1, t):
                    copy.start()

            if c == 0:
                follow()
            else:
                pl.when(k + 1 < steps)(follow)
            return 0

        lax.fori_loop(0, slices, slab, 0)

    for way in range(2):
        loads[way].wait()
        for h in range(nh):
            send_first(1, way, h)
    loads[2].wait()
    for t in range(slices):
        for h in range(nh):
            products(0, 1, t, h, load(g, 1, t, h))
        for copy in side(0, t):
            copy.start()

    for way in range(2):
        loads[3 + way].wait()
        for h in range(nh):
            send_first(0, way, h)

    def iteration(n, _):
        half_sweep(n, 0)
        half_sweep(n, 1)
        return 0

    lax.fori_loop(0, ITERS, iteration, 0)

    spot = lax.broadcasted_iota(jnp.int32, (1, LANES), 1)
    sums = jnp.zeros((1, LANES), jnp.float32)
    for n in range(ITERS):
        for part in range(2):
            value = jnp.sum(jnp.sum(mon[n, part], axis=0, keepdims=True), axis=1, keepdims=True)
            sums = jnp.where(spot == 2 * n + part, value, sums)

    lines = plane.shape[0]
    here = (me["ta"] * sizes["gz"] + me["gz"]) * sizes["gy"] + me["gy"]
    plane[here] = sums
    offsets = [
        (i, j, k)
        for i in range(sizes["ta"])
        for j in range(sizes["gz"])
        for k in range(sizes["gy"])
        if i or j or k
    ]

    def to_other(i, j, k):
        return pltpu.make_async_remote_copy(
            src_ref=plane.at[here],
            dst_ref=plane.at[here],
            send_sem=red_send,
            recv_sem=red_recv,
            device_id=peer("ta", i) | peer("gz", j) | peer("gy", k),
            device_id_type=MESH,
        )

    for offset in reversed(offsets):
        to_other(*offset).start()
    width = sizes["gz"] * sizes["gy"]
    arrivals = pltpu.make_async_remote_copy(
        src_ref=plane.at[pl.ds(0, lines - 1)],
        dst_ref=plane.at[pl.ds(0, lines - 1)],
        send_sem=red_send,
        recv_sem=red_recv,
        device_id=peer("ta", 1),
        device_id_type=MESH,
    )
    for t in range(slices):
        for h in range(nh):
            turn_own(steps - 1, 1, t, t, h)
    arrivals.wait_recv()
    sums = total([plane[number] for number in range(lines)])
    sites = slices * depth * row_len * sizes["ta"] * width
    for n in range(ITERS):
        mon_out[0, n] = 1.0 - sums[0, 2 * n] / (24.0 * sites)
        mon_out[1, n] = sums[0, 2 * n + 1] / float(sites)
    arrivals.wait_send()
    for h in range(nh):
        for way in range(2):
            for colour in range(2):
                first_copy(colour, way, h).wait_send()
            for k in range(steps - 1):
                t_copy(k, way, h).wait_send()
    for k in range(steps):
        for t in range(slices):
            for copy in side(k, t):
                copy.wait_send()


def shards(sizes, lattice_links, transform):
    slices, depth, row_len = transform.shape[2:]
    nh = row_len // LANES
    strips = LANES // (NX // 2)
    groups = -(-18 // strips)
    steps = 2 * ITERS
    face = (18, slices, depth, row_len)
    assert depth == 8 and slices == 2 and row_len % LANES == 0
    f32 = jnp.float32
    width = sizes["gz"] * sizes["gy"]
    lines = width * sizes["ta"]
    g, mon = pl.pallas_call(
        functools.partial(kernel, sizes),
        out_shape=(
            pltpu.VMEM(transform.shape, f32),
            pltpu.SMEM((2, ITERS), f32),
        ),
        in_specs=[pl.BlockSpec(memory_space=pltpu.HBM)] * 2,
        out_specs=(
            pl.BlockSpec(memory_space=pltpu.VMEM),
            pl.BlockSpec(memory_space=pltpu.SMEM),
        ),
        scratch_shapes=[
            pltpu.VMEM(lattice_links.shape, f32),
            pltpu.VMEM(face, f32),
            pltpu.VMEM((2, 18, depth, row_len), f32),
            pltpu.VMEM(face, f32),
            pltpu.VMEM(face, f32),
            pltpu.VMEM((steps, 2, 12, depth, row_len), f32),
            pltpu.VMEM((steps, 2, 12, depth, row_len), f32),
            pltpu.VMEM((2, 2, 18, depth, row_len), f32),
            pltpu.VMEM((2, 2, 8, depth, row_len), f32),
            pltpu.VMEM((2, 2, 8, depth, row_len), f32),
            pltpu.VMEM((steps, 2, slices, 18, row_len), f32),
            pltpu.VMEM((steps, 2, slices, 18, row_len), f32),
            pltpu.VMEM((steps, 2, slices, groups, depth, LANES), f32),
            pltpu.VMEM((steps, 2, slices, groups, depth, LANES), f32),
            pltpu.VMEM((ITERS, 2, depth, LANES), f32),
            pltpu.VMEM((lines, 1, LANES), f32),
            pltpu.SemaphoreType.DMA((7,)),
            pltpu.SemaphoreType.DMA((steps - 1, 2, nh)),
            pltpu.SemaphoreType.DMA((steps - 1, 2, nh)),
            pltpu.SemaphoreType.DMA((2, 2, nh)),
            pltpu.SemaphoreType.DMA((2, 2, nh)),
            pltpu.SemaphoreType.DMA((steps, 4, slices)),
            pltpu.SemaphoreType.DMA((steps, 4, slices)),
            pltpu.SemaphoreType.DMA,
            pltpu.SemaphoreType.DMA,
        ],
        compiler_params=pltpu.CompilerParams(
            collective_id=0, has_side_effects=True, vmem_limit_bytes=67043328 - 900000 // 4096 * 4096
        ),
    )(lattice_links, transform)

    def finish(g_ref, mon_ref, out_ref, mon_out, sem, sem2):
        copy = pltpu.make_async_copy(g_ref, out_ref, sem)
        copy.start()
        small = pltpu.make_async_copy(mon_ref, mon_out, sem2)
        small.start()
        copy.wait()
        small.wait()

    return pl.pallas_call(
        finish,
        out_shape=(
            jax.ShapeDtypeStruct(transform.shape, f32),
            jax.ShapeDtypeStruct((2, ITERS), f32),
        ),
        in_specs=[pl.BlockSpec(memory_space=pltpu.VMEM), pl.BlockSpec(memory_space=pltpu.SMEM)],
        out_specs=(pl.BlockSpec(memory_space=pltpu.HBM), pl.BlockSpec(memory_space=pltpu.HBM)),
        scratch_shapes=[pltpu.SemaphoreType.DMA,pltpu.SemaphoreType.DMA],
        compiler_params=pltpu.CompilerParams(vmem_limit_bytes=1 << 20),
    )(g, mon)


def solution(mesh):
    sizes = {axis: mesh.shape[axis] for axis in AXES}
    return jax.shard_map(
        functools.partial(shards, sizes),
        mesh=mesh,
        in_specs=(P(None, None, None, "ta", "gz", "gy"), P(None, None, "ta", "gz", "gy")),
        out_specs=(P(None, None, "ta", "gz", "gy"), P()),
        check_vma=False,
    )
```

```python
import functools

import jax
import jax.numpy as jnp
from jax import lax
from jax.experimental import pallas as pl
from jax.experimental.pallas import tpu as pltpu
from jax.sharding import PartitionSpec as P

NX = 64
ITERS = 2
OMEGA = 1.7
GUARD = 1e-12
FLOOR = 1e-20
FAR = 1e15
LANES = 128
AXES = ("ta", "gz", "gy")
MESH = pl.DeviceIdType.MESH


def total(terms):
    out = terms[0]
    for term in terms[1:]:
        out = out + term
    return out


def mul(a, b):
    re, im = [], []
    for i in range(3):
        for j in range(3):
            re.append(
                total([a[3 * i + k] * b[3 * k + j] for k in range(3)])
                - total([a[9 + 3 * i + k] * b[9 + 3 * k + j] for k in range(3)])
            )
            im.append(
                total([a[3 * i + k] * b[9 + 3 * k + j] for k in range(3)])
                + total([a[9 + 3 * i + k] * b[3 * k + j] for k in range(3)])
            )
    return re + im


def mul_adj(a, b):
    re, im = [], []
    for i in range(3):
        for j in range(3):
            re.append(
                total([a[3 * i + k] * b[3 * j + k] for k in range(3)])
                + total([a[9 + 3 * i + k] * b[9 + 3 * j + k] for k in range(3)])
            )
            im.append(
                total([a[9 + 3 * i + k] * b[3 * j + k] for k in range(3)])
                - total([a[3 * i + k] * b[9 + 3 * j + k] for k in range(3)])
            )
    return re + im


def add(a, b):
    return [x + y for x, y in zip(a, b)]


def add_adj(a, b):
    out = []
    for i in range(3):
        for j in range(3):
            out.append(a[3 * i + j] + b[3 * j + i])
    for i in range(3):
        for j in range(3):
            out.append(a[9 + 3 * i + j] - b[9 + 3 * j + i])
    return out


def rotation(a, i, j):
    ii, jj, ij, ji = 4 * i, 4 * j, 3 * i + j, 3 * j + i
    v0 = a[ii] + a[jj]
    v1 = -(a[9 + ij] + a[9 + ji])
    v2 = a[ji] - a[ij]
    v3 = a[9 + jj] - a[9 + ii]
    tail = v1 * v1 + v2 * v2 + v3 * v3
    length = jnp.sqrt(v0 * v0 + tail)
    s0 = (1.0 - OMEGA) * length + OMEGA * v0
    inv = lax.rsqrt(s0 * s0 + (OMEGA * OMEGA) * tail + GUARD)
    scaled = OMEGA * inv
    return (s0 * inv, v1 * scaled, v2 * scaled, v3 * scaled)


def rotate(m, q, i, j):
    q0, q1, q2, q3 = q
    out = list(m)
    for k in range(3):
        ur, ui = m[3 * i + k], m[9 + 3 * i + k]
        lr, li = m[3 * j + k], m[9 + 3 * j + k]
        out[3 * i + k] = q0 * ur - q3 * ui + q2 * lr - q1 * li
        out[9 + 3 * i + k] = q0 * ui + q3 * ur + q2 * li + q1 * lr
        out[3 * j + k] = q0 * lr + q3 * li - q2 * ur - q1 * ui
        out[9 + 3 * j + k] = q0 * li - q3 * lr - q2 * ui + q1 * ur
    return out


def third_row(m):
    re, im = list(m[:6]), list(m[6:])
    for k in range(3):
        a, b = (k + 1) % 3, (k + 2) % 3
        re.append(
            m[a] * m[3 + b] - m[6 + a] * m[9 + b] - m[b] * m[3 + a] + m[6 + b] * m[9 + a]
        )
        im.append(
            m[b] * m[9 + a] + m[6 + b] * m[3 + a] - m[a] * m[9 + b] - m[6 + a] * m[3 + b]
        )
    return re + im


def to_flat(x, v):
    square = total([c * c for c in v])
    scale = jnp.where(x >= 0.0, 1.0 + x, square / (1.0 + jnp.abs(x)))
    pole = scale < FLOOR
    inv = 1.0 / jnp.where(pole, 1.0, scale)
    flat = [c * inv for c in v]
    return [jnp.where(pole, FAR, flat[0])] + [jnp.where(pole, 0.0, c) for c in flat[1:]]


def from_flat(flat):
    scale = 2.0 / (1.0 + total([c * c for c in flat]))
    return [scale - 1.0] + [c * scale for c in flat]


def cmul(a, b):
    return (a[0] * b[0] - a[1] * b[1], a[0] * b[1] + a[1] * b[0])


def cmul_conj(a, b):
    return (a[0] * b[0] + a[1] * b[1], a[1] * b[0] - a[0] * b[1])


def first_row(flat):
    r0, i0, r1, i1, r2, i2 = from_flat(flat)
    square = r0 * r0 + i0 * i0 + r1 * r1 + i1 * i1
    small = square < FLOOR
    inv = lax.rsqrt(jnp.where(small, 1.0, square))
    c0 = (jnp.where(small, 1.0, r0 * inv), jnp.where(small, 0.0, i0 * inv))
    c1 = (jnp.where(small, 0.0, r1 * inv), jnp.where(small, 0.0, i1 * inv))
    norm = jnp.where(small, 0.0, square * inv)
    return [r0, r1, r2], [i0, i1, i2], c0, c1, norm


def encode(m):
    flat = to_flat(m[0], [m[9], m[1], m[10], m[2], m[11]])
    re, im, c0, c1, norm = first_row(flat)
    a2 = (re[2], im[2])
    b0, b1, b2 = [(m[3 + k], m[12 + k]) for k in range(3)]
    x, y = cmul(b1, c0), cmul(b0, c1)
    u, v = cmul_conj(b0, c0), cmul_conj(b1, c1)
    w = cmul(a2, (u[0] + v[0], u[1] + v[1]))
    return flat + to_flat(
        x[0] - y[0], [x[1] - y[1], norm * b2[0] - w[0], norm * b2[1] - w[1]]
    )


def decode(values):
    re, im, c0, c1, norm = first_row(values[:5])
    p0, p1, r0, r1 = from_flat(values[5:])
    p, r = (p0, p1), (r0, r1)
    turn = cmul_conj(r, (re[2], im[2]))
    x, y = cmul_conj(p, c1), cmul(turn, c0)
    u, v = cmul_conj(p, c0), cmul(turn, c1)
    return third_row(
        re + [-x[0] - y[0], u[0] - v[0], norm * r0]
        + im + [-x[1] - y[1], u[1] - v[1], norm * r1]
    )


PAIRS = ((0, 1), (0, 2), (1, 2))


def kernel(
    sizes,
    links_hbm,
    trans_hbm,
    g,
    mon_out,
    links,
    w,
    cb,
    py,
    pz,
    tsend,
    trecv,
    halo,
    esend,
    erecv,
    zsend,
    zrecv,
    ysend,
    yrecv,
    mon,
    plane,
    load_sem,
    t_send_sem,
    t_recv_sem,
    first_send_sem,
    first_recv_sem,
    side_send_sem,
    side_recv_sem,
    red_send,
    red_recv,
):
    slices, depth, row_len = g.shape[2:]
    nh = row_len // LANES
    half = NX // 2
    strips = LANES // half
    groups = ysend.shape[3]
    last = slices - 1
    steps = 2 * ITERS
    me = {a: lax.axis_index(a) for a in AXES}

    def peer(axis, d):
        n = sizes[axis]
        return {axis: lax.rem(me[axis] + d + n, n)}

    loads = [
        pltpu.make_async_copy(src, dst, load_sem.at[number])
        for number, (src, dst) in enumerate(
            [
                (trans_hbm.at[1], g.at[1]),
                (links_hbm.at[1, 3], links.at[1, 3]),
                (links_hbm.at[1, pl.ds(1, 2)], links.at[1, pl.ds(1, 2)]),
                (trans_hbm.at[0], g.at[0]),
                (links_hbm.at[0, 3], links.at[0, 3]),
                (links_hbm.at[1, 0], links.at[1, 0]),
                (links_hbm.at[0, pl.ds(0, 3)], links.at[0, pl.ds(0, 3)]),
            ]
        )
    ]
    for copy in loads:
        copy.start()
    barrier = pltpu.get_barrier_semaphore()
    near = [(a, d) for a in AXES for d in sorted({1, sizes[a] - 1})]
    for axis, d in near:
        pl.semaphore_signal(barrier, inc=1, device_id=peer(axis, d), device_id_type=MESH)
    mon[...] = jnp.zeros_like(mon)
    pl.semaphore_wait(barrier, len(near))

    row = lax.broadcasted_iota(jnp.int32, (depth, LANES), 0)
    lane = lax.broadcasted_iota(jnp.int32, (depth, LANES), 1)
    column = lane % half
    strip = lane // half
    flip = 1 - lax.rem(me["ta"], 2)

    def piece(h):
        return pl.ds(h * LANES if isinstance(h, int) else pl.multiple_of(h * LANES, LANES), LANES)

    def load(ref, *index):
        t, h = index[-2:]
        return [ref[index[:-2] + (comp, t, slice(None), piece(h))] for comp in range(18)]

    def store(ref, values, *index):
        t, h = index[-2:]
        for comp in range(18):
            ref[index[:-2] + (comp, t, slice(None), piece(h))] = values[comp]

    def put(ref, index, h, values):
        for number, value in enumerate(values):
            ref[index + (number, slice(None), piece(h))] = value

    def get(ref, index, h, count):
        return [ref[index + (number, slice(None), piece(h))] for number in range(count)]

    def along_t(way):
        return {"ta": lax.rem(me["ta"] + 2 * way - 1 + sizes["ta"], sizes["ta"])}

    def t_copy(slot, way, h):
        return pltpu.make_async_remote_copy(
            src_ref=tsend.at[slot, way, :, :, piece(h)],
            dst_ref=trecv.at[slot, way, :, :, piece(h)],
            send_sem=t_send_sem.at[slot % 2, way, h],
            recv_sem=t_recv_sem.at[slot % 2, way, h],
            device_id=along_t(way),
            device_id_type=MESH,
        )

    def first_copy(colour, way, h):
        return pltpu.make_async_remote_copy(
            src_ref=esend.at[colour, way, :, :, piece(h)],
            dst_ref=erecv.at[colour, way, :, :, piece(h)],
            send_sem=first_send_sem.at[colour, way, h],
            recv_sem=first_recv_sem.at[colour, way, h],
            device_id=along_t(way),
            device_id_type=MESH,
        )

    def send_first(colour, way, h):
        values = load(g, colour, last if way else 0, h)
        if way:
            values = mul(values, load(links, colour, 3, last, h))
        put(esend, (colour, way), h, encode(values))
        first_copy(colour, way, h).start()

    def take_first(colour, way, h):
        first_copy(colour, way, h).wait()
        m = decode(get(erecv, (colour, way), h, 8))
        put(halo, (colour, way), h, m)
        return m

    def side(k, t):
        ends = [(zsend, zrecv, "gz"), (ysend, yrecv, "gy")]
        return [
            pltpu.make_async_remote_copy(
                src_ref=src.at[k, way, t],
                dst_ref=dst.at[k, way, t],
                send_sem=side_send_sem.at[k % 2, 2 * number + way, t],
                recv_sem=side_recv_sem.at[k % 2, 2 * number + way, t],
                device_id=peer(axis, 1 if way else -1),
                device_id_type=MESH,
            )
            for number, (src, dst, axis) in enumerate(ends)
            for way in range(2)
        ]

    def pack(values, ref, k, way, t):
        for group in range(groups):
            tile = None
            for j in range(strips):
                comp = group * strips + j
                if comp >= 18:
                    continue
                turn = (half * (j + way)) % LANES
                moved = pltpu.roll(values[comp], turn, 1) if turn else values[comp]
                tile = moved if tile is None else jnp.where(strip == j, moved, tile)
            ref[k, way, t, group] = tile

    def unpack(ref, k, way, t):
        out = []
        for comp in range(18):
            group, j = comp // strips, comp % strips
            tile = ref[k, way, t, group]
            turn = (LANES - half - half * j if way == 0 else LANES - half * j) % LANES
            out.append(pltpu.roll(tile, turn, 1) if turn else tile)
        return out

    def products(k, p, t, h, other):
        prod_y = mul(other, load(links, p, 1, t, h))
        store(py, prod_y, t, h)
        if h == 0:
            pack(other, ysend, k, 0, t)
        if h == nh - 1:
            pack(prod_y, ysend, k, 1, t)
        prod_z = mul(other, load(links, p, 2, t, h))
        store(pz, prod_z, t, h)
        for comp in range(18):
            zsend[k, 0, t, comp : comp + 1, piece(h)] = other[comp][0:1]
            zsend[k, 1, t, comp : comp + 1, piece(h)] = prod_z[comp][depth - 1 : depth]

    def turn_own(k, c, t, way, h):
        q = get(tsend, (k, way), h, 12)
        own = load(g, c, t, h)
        for number, (i, j) in enumerate(PAIRS):
            own = rotate(own, q[4 * number : 4 * number + 4], i, j)
        store(g, own, c, t, h)
        return own

    def half_sweep(n, c):
        p = 1 - c
        k = 2 * n + c
        if c == 0:
            @pl.when(n == 0)
            def _():
                for copy in loads[5:]:
                    copy.wait()

        def inside(h, _):
            for t in range(slices):
                offset = (row + strip + (t + c)) % 2
                other = load(g, p, t, h)
                ahead = []
                for v in other:
                    stepped = jnp.where(
                        column == half - 1, pltpu.roll(v, half - 1, 1), pltpu.roll(v, LANES - 1, 1)
                    )
                    ahead.append(jnp.where(offset == 0, v, stepped))
                acc = mul_adj(load(links, c, 0, t, h), ahead)
                behind = []
                for v in mul(other, load(links, p, 0, t, h)):
                    stepped = jnp.where(
                        column == 0, pltpu.roll(v, LANES - half + 1, 1), pltpu.roll(v, 1, 1)
                    )
                    behind.append(jnp.where(offset == 0, stepped, v))
                acc = add_adj(acc, behind)
                if t < last:
                    acc = add(acc, mul_adj(load(links, c, 3, t, h), load(g, p, t + 1, h)))
                if t > 0:
                    acc = add_adj(acc, mul(load(g, p, t - 1, h), load(links, p, 3, t - 1, h)))
                store(w, acc, t, h)

            def outer():
                return (
                    mul(load(g, c, last, h), load(links, c, 3, last, h)),
                    load(g, c, 0, h),
                )

            def turned_halo(way):
                m = get(halo, (p, way), h, 18)
                q = get(trecv, (k - 3, way), h, 12)
                for number, (i, j) in enumerate(PAIRS):
                    m = rotate(m, q[4 * number : 4 * number + 4], i, j)
                put(halo, (p, way), h, m)
                return m

            def prepare(*halos):
                for way, values in enumerate(outer()):
                    if halos:
                        values = mul_adj(halos[0](way), values)
                    put(cb, (way,), h, values)

            if c == 0:
                pl.when(n == 0)(lambda: prepare())
                pl.when(n == 1)(lambda: prepare(lambda way: get(halo, (p, way), h, 18)))
                if ITERS > 2:
                    pl.when(n > 1)(lambda: prepare(turned_halo))
            else:
                pl.when(n == 0)(lambda: prepare(lambda way: take_first(p, way, h)))
                pl.when(n > 0)(lambda: prepare(turned_halo))
            return 0

        lax.fori_loop(0, nh, inside, 0)

        def along_yz(t, h):
            acc = load(w, t, h)
            behind, ahead = [], []
            prod_z = load(pz, t, h)
            other = load(g, p, t, h)
            for comp in range(18):
                edge = zrecv[k, 0, t, comp : comp + 1, piece(h)]
                edge = jnp.broadcast_to(edge, (depth, LANES))
                moved = pltpu.roll(other[comp], depth - 1, 0)
                ahead.append(jnp.where(row == depth - 1, edge, moved))
                edge = zrecv[k, 1, t, comp : comp + 1, piece(h)]
                edge = jnp.broadcast_to(edge, (depth, LANES))
                behind.append(jnp.where(row == 0, edge, pltpu.roll(prod_z[comp], 1, 0)))
            acc = add_adj(acc, behind)
            acc = add(acc, mul_adj(load(links, c, 2, t, h), ahead))
            if h == nh - 1:
                edge = unpack(yrecv, k, 0, t)
            else:
                edge = [pltpu.roll(v, LANES - half, 1) for v in load(g, p, t, h + 1)]
            ahead = [
                jnp.where(strip == strips - 1, e, pltpu.roll(v, LANES - half, 1))
                for e, v in zip(edge, other)
            ]
            acc = add(acc, mul_adj(load(links, c, 1, t, h), ahead))
            if h == 0:
                edge = unpack(yrecv, k, 1, t)
            else:
                edge = [pltpu.roll(v, half, 1) for v in load(py, t, h - 1)]
            behind = [
                jnp.where(strip == 0, e, pltpu.roll(v, half, 1))
                for e, v in zip(edge, load(py, t, h))
            ]
            acc = add_adj(acc, behind)
            store(w, mul(load(g, c, t, h), acc), t, h)

        def take(way, h):
            def turn():
                t_copy(k - 1, way, h).wait()
                q = get(trecv, (k - 1, way), h, 12)
                m = get(cb, (way,), h, 18)
                for number, (i, j) in enumerate(PAIRS):
                    m = rotate(m, q[4 * number : 4 * number + 4], i, j)
                put(cb, (way,), h, m)

            if c == 1:
                turn()
                return

            @pl.when(n == 0)
            def _():
                put(cb, (way,), h, mul_adj(take_first(p, way, h), get(cb, (way,), h, 18)))

            pl.when(n > 0)(turn)

        def monitor(a):
            func = a[0] + a[4] + a[8]
            mean = (a[9] + a[13] + a[17]) * (1.0 / 3.0)
            div = None
            for i in range(3):
                d = a[9 + 4 * i] - mean
                div = d * d if div is None else div + d * d
            for i, j in PAIRS:
                d = a[3 * i + j] - a[3 * j + i]
                e = a[9 + 3 * i + j] + a[9 + 3 * j + i]
                div = div + 0.5 * (d * d + e * e)
            mon[n, 0] += func
            mon[n, 1] += div

        def slab(number, _):
            back = (number + flip) % 2
            ahead = 1 - back
            t = ahead * last
            for copy in side(k, t):
                copy.wait()
            for h in range(nh):
                along_yz(t, h)
            for h in range(nh):
                take(back, h)
                a = add_adj(load(w, t, h), get(cb, (back,), h, 18))
                turns = []
                for i, j in PAIRS:
                    q = rotation(a, i, j)
                    turns.extend(q)
                    a = rotate(a, q, i, j)
                put(tsend, (k, ahead), h, turns)

                if c == 0:
                    t_copy(k, ahead, h).start()
                    products(k + 1, c, t, h, turn_own(k, c, t, ahead, h))
                else:
                    @pl.when(k + 1 < steps)
                    def _():
                        t_copy(k, ahead, h).start()

                    monitor(a)

                    @pl.when(k + 1 < steps)
                    def _():
                        products(k + 1, c, t, h, turn_own(k, c, t, ahead, h))

            def follow():
                for copy in side(k + 1, t):
                    copy.start()

            if c == 0:
                follow()
            else:
                pl.when(k + 1 < steps)(follow)
            return 0

        lax.fori_loop(0, slices, slab, 0)

    def send_both(colour):
        for order in range(2):
            @pl.when(flip == 1 - order)
            def _():
                for way in (order, 1 - order):
                    for h in range(nh):
                        send_first(colour, way, h)

    loads[0].wait()
    loads[1].wait()
    send_both(1)
    loads[2].wait()
    for t in range(slices):
        for h in range(nh):
            products(0, 1, t, h, load(g, 1, t, h))
        for copy in side(0, t):
            copy.start()

    loads[3].wait()
    loads[4].wait()
    send_both(0)

    def iteration(n, _):
        half_sweep(n, 0)
        half_sweep(n, 1)
        return 0

    lax.fori_loop(0, ITERS, iteration, 0)

    spot = lax.broadcasted_iota(jnp.int32, (1, LANES), 1)
    sums = jnp.zeros((1, LANES), jnp.float32)
    for n in range(ITERS):
        for part in range(2):
            value = jnp.sum(jnp.sum(mon[n, part], axis=0, keepdims=True), axis=1, keepdims=True)
            sums = jnp.where(spot == 2 * n + part, value, sums)

    lines = plane.shape[0]
    here = (me["ta"] * sizes["gz"] + me["gz"]) * sizes["gy"] + me["gy"]
    plane[here] = sums
    offsets = [
        (i, j, k)
        for i in range(sizes["ta"])
        for j in range(sizes["gz"])
        for k in range(sizes["gy"])
        if i or j or k
    ]

    toward = 1 - 2 * (2 * me["ta"] // sizes["ta"])

    def to_other(i, j, k):
        return pltpu.make_async_remote_copy(
            src_ref=plane.at[here],
            dst_ref=plane.at[here],
            send_sem=red_send,
            recv_sem=red_recv,
            device_id=peer("ta", i) | peer("gz", j) | peer("gy", k),
            device_id_type=MESH,
        )

    for offset in reversed(offsets):
        to_other(*offset).start()
    width = sizes["gz"] * sizes["gy"]
    arrivals = pltpu.make_async_remote_copy(
        src_ref=plane.at[pl.ds(0, lines - 1)],
        dst_ref=plane.at[pl.ds(0, lines - 1)],
        send_sem=red_send,
        recv_sem=red_recv,
        device_id=peer("ta", 1),
        device_id_type=MESH,
    )
    for t in range(slices):
        for h in range(nh):
            turn_own(steps - 1, 1, t, t, h)
    arrivals.wait_send()
    arrivals.wait_recv()
    sums = total([plane[number] for number in range(lines)])
    sites = slices * depth * row_len * sizes["ta"] * width
    for n in range(ITERS):
        mon_out[0, n] = 1.0 - sums[0, 2 * n] / (24.0 * sites)
        mon_out[1, n] = sums[0, 2 * n + 1] / float(sites)


def shards(sizes, lattice_links, transform):
    slices, depth, row_len = transform.shape[2:]
    nh = row_len // LANES
    strips = LANES // (NX // 2)
    groups = -(-18 // strips)
    steps = 2 * ITERS
    face = (18, slices, depth, row_len)
    assert depth == 8 and slices == 2 and row_len % LANES == 0
    f32 = jnp.float32
    width = sizes["gz"] * sizes["gy"]
    lines = width * sizes["ta"]
    g, mon = pl.pallas_call(
        functools.partial(kernel, sizes),
        out_shape=(
            pltpu.VMEM(transform.shape, f32),
            pltpu.SMEM((2, ITERS), f32),
        ),
        in_specs=[pl.BlockSpec(memory_space=pltpu.HBM)] * 2,
        out_specs=(
            pl.BlockSpec(memory_space=pltpu.VMEM),
            pl.BlockSpec(memory_space=pltpu.SMEM),
        ),
        scratch_shapes=[
            pltpu.VMEM(lattice_links.shape, f32),
            pltpu.VMEM(face, f32),
            pltpu.VMEM((2, 18, depth, row_len), f32),
            pltpu.VMEM(face, f32),
            pltpu.VMEM(face, f32),
            pltpu.VMEM((steps, 2, 12, depth, row_len), f32),
            pltpu.VMEM((steps, 2, 12, depth, row_len), f32),
            pltpu.VMEM((2, 2, 18, depth, row_len), f32),
            pltpu.VMEM((2, 2, 8, depth, row_len), f32),
            pltpu.VMEM((2, 2, 8, depth, row_len), f32),
            pltpu.VMEM((steps, 2, slices, 18, row_len), f32),
            pltpu.VMEM((steps, 2, slices, 18, row_len), f32),
            pltpu.VMEM((steps, 2, slices, groups, depth, LANES), f32),
            pltpu.VMEM((steps, 2, slices, groups, depth, LANES), f32),
            pltpu.VMEM((ITERS, 2, depth, LANES), f32),
            pltpu.VMEM((lines, 1, LANES), f32),
            pltpu.SemaphoreType.DMA((7,)),
            pltpu.SemaphoreType.DMA((2, 2, nh)),
            pltpu.SemaphoreType.DMA((2, 2, nh)),
            pltpu.SemaphoreType.DMA((2, 2, nh)),
            pltpu.SemaphoreType.DMA((2, 2, nh)),
            pltpu.SemaphoreType.DMA((2, 4, slices)),
            pltpu.SemaphoreType.DMA((2, 4, slices)),
            pltpu.SemaphoreType.DMA,
            pltpu.SemaphoreType.DMA,
        ],
        compiler_params=pltpu.CompilerParams(
            collective_id=0, has_side_effects=True, vmem_limit_bytes=67043328 - 900000 // 4096 * 4096
        ),
    )(lattice_links, transform)

    def finish(g_ref, mon_ref, out_ref, mon_out, sem, sem2):
        copy = pltpu.make_async_copy(g_ref, out_ref, sem)
        copy.start()
        small = pltpu.make_async_copy(mon_ref, mon_out, sem2)
        small.start()
        copy.wait()
        small.wait()

    return pl.pallas_call(
        finish,
        out_shape=(
            jax.ShapeDtypeStruct(transform.shape, f32),
            jax.ShapeDtypeStruct((2, ITERS), f32),
        ),
        in_specs=[pl.BlockSpec(memory_space=pltpu.VMEM), pl.BlockSpec(memory_space=pltpu.SMEM)],
        out_specs=(pl.BlockSpec(memory_space=pltpu.HBM), pl.BlockSpec(memory_space=pltpu.HBM)),
        scratch_shapes=[pltpu.SemaphoreType.DMA,pltpu.SemaphoreType.DMA],
        compiler_params=pltpu.CompilerParams(vmem_limit_bytes=1 << 20),
    )(g, mon)


def solution(mesh):
    sizes = {axis: mesh.shape[axis] for axis in AXES}
    return jax.shard_map(
        functools.partial(shards, sizes),
        mesh=mesh,
        in_specs=(P(None, None, None, "ta", "gz", "gy"), P(None, None, "ta", "gz", "gy")),
        out_specs=(P(None, None, "ta", "gz", "gy"), P()),
        check_vma=False,
    )
```

```python
import functools

import jax
import jax.numpy as jnp
from jax import lax
from jax.experimental import pallas as pl
from jax.experimental.pallas import tpu as pltpu
from jax.sharding import PartitionSpec as P

NX = 64
ITERS = 2
OMEGA = 1.7
GUARD = 1e-12
FLOOR = 1e-20
FAR = 1e15
LANES = 128
AXES = ("ta", "gz", "gy")
MESH = pl.DeviceIdType.MESH


def total(terms):
    out = terms[0]
    for term in terms[1:]:
        out = out + term
    return out


def mul(a, b):
    re, im = [], []
    for i in range(3):
        for j in range(3):
            re.append(
                total([a[3 * i + k] * b[3 * k + j] for k in range(3)])
                - total([a[9 + 3 * i + k] * b[9 + 3 * k + j] for k in range(3)])
            )
            im.append(
                total([a[3 * i + k] * b[9 + 3 * k + j] for k in range(3)])
                + total([a[9 + 3 * i + k] * b[3 * k + j] for k in range(3)])
            )
    return re + im


def mul_adj(a, b):
    re, im = [], []
    for i in range(3):
        for j in range(3):
            re.append(
                total([a[3 * i + k] * b[3 * j + k] for k in range(3)])
                + total([a[9 + 3 * i + k] * b[9 + 3 * j + k] for k in range(3)])
            )
            im.append(
                total([a[9 + 3 * i + k] * b[3 * j + k] for k in range(3)])
                - total([a[3 * i + k] * b[9 + 3 * j + k] for k in range(3)])
            )
    return re + im


def add(a, b):
    return [x + y for x, y in zip(a, b)]


def add_adj(a, b):
    out = []
    for i in range(3):
        for j in range(3):
            out.append(a[3 * i + j] + b[3 * j + i])
    for i in range(3):
        for j in range(3):
            out.append(a[9 + 3 * i + j] - b[9 + 3 * j + i])
    return out


def rotation(a, i, j):
    ii, jj, ij, ji = 4 * i, 4 * j, 3 * i + j, 3 * j + i
    v0 = a[ii] + a[jj]
    v1 = -(a[9 + ij] + a[9 + ji])
    v2 = a[ji] - a[ij]
    v3 = a[9 + jj] - a[9 + ii]
    tail = v1 * v1 + v2 * v2 + v3 * v3
    length = jnp.sqrt(v0 * v0 + tail)
    s0 = (1.0 - OMEGA) * length + OMEGA * v0
    inv = lax.rsqrt(s0 * s0 + (OMEGA * OMEGA) * tail + GUARD)
    scaled = OMEGA * inv
    return (s0 * inv, v1 * scaled, v2 * scaled, v3 * scaled)


def rotate(m, q, i, j):
    q0, q1, q2 = q[:3]
    out = list(m)
    for k in range(3):
        ur, ui = m[3 * i + k], m[9 + 3 * i + k]
        lr, li = m[3 * j + k], m[9 + 3 * j + k]
        values = [
            q0 * ur + q2 * lr - q1 * li,
            q0 * ui + q2 * li + q1 * lr,
            q0 * lr - q2 * ur - q1 * ui,
            q0 * li - q2 * ui + q1 * ur,
        ]
        if len(q) == 4:
            turned = [-ui, ur, li, -lr]
            values = [v + q[3] * u for v, u in zip(values, turned)]
        out[3 * i + k], out[9 + 3 * i + k] = values[:2]
        out[3 * j + k], out[9 + 3 * j + k] = values[2:]
    return out


PARTS = (slice(0, 3), slice(3, 7), slice(7, 11))


def turn(m, q):
    for part, (i, j) in zip(PARTS, PAIRS):
        m = rotate(m, q[part], i, j)
    return m


def reduced(first, second, third):
    r0, r1, r2, r3 = first
    square = r0 * r0 + r3 * r3
    small = square < FLOOR
    inv = lax.rsqrt(jnp.where(small, 1.0, square))
    phase = (jnp.where(small, 1.0, r0 * inv), jnp.where(small, 0.0, -r3 * inv))
    back = (phase[0], -phase[1])
    a2, a1 = cmul(phase, (r2, r1))
    b0, b3 = cmul(back, (second[0], second[3]))
    c0, c3 = cmul(phase, (third[0], third[3]))
    c2, c1 = cmul(back, (third[2], third[1]))
    return [square * inv, a1, a2, b0, second[1], second[2], b3, c0, c1, c2, c3]


def third_row(m):
    re, im = list(m[:6]), list(m[6:])
    for k in range(3):
        a, b = (k + 1) % 3, (k + 2) % 3
        re.append(
            m[a] * m[3 + b] - m[6 + a] * m[9 + b] - m[b] * m[3 + a] + m[6 + b] * m[9 + a]
        )
        im.append(
            m[b] * m[9 + a] + m[6 + b] * m[3 + a] - m[a] * m[9 + b] - m[6 + a] * m[3 + b]
        )
    return re + im


def to_flat(x, v):
    square = total([c * c for c in v])
    scale = jnp.where(x >= 0.0, 1.0 + x, square / (1.0 + jnp.abs(x)))
    pole = scale < FLOOR
    inv = 1.0 / jnp.where(pole, 1.0, scale)
    flat = [c * inv for c in v]
    return [jnp.where(pole, FAR, flat[0])] + [jnp.where(pole, 0.0, c) for c in flat[1:]]


def from_flat(flat):
    scale = 2.0 / (1.0 + total([c * c for c in flat]))
    return [scale - 1.0] + [c * scale for c in flat]


def cmul(a, b):
    return (a[0] * b[0] - a[1] * b[1], a[0] * b[1] + a[1] * b[0])


def cmul_conj(a, b):
    return (a[0] * b[0] + a[1] * b[1], a[1] * b[0] - a[0] * b[1])


def first_row(flat):
    r0, i0, r1, i1, r2, i2 = from_flat(flat)
    square = r0 * r0 + i0 * i0 + r1 * r1 + i1 * i1
    small = square < FLOOR
    inv = lax.rsqrt(jnp.where(small, 1.0, square))
    c0 = (jnp.where(small, 1.0, r0 * inv), jnp.where(small, 0.0, i0 * inv))
    c1 = (jnp.where(small, 0.0, r1 * inv), jnp.where(small, 0.0, i1 * inv))
    norm = jnp.where(small, 0.0, square * inv)
    return [r0, r1, r2], [i0, i1, i2], c0, c1, norm


def encode(m):
    flat = to_flat(m[0], [m[9], m[1], m[10], m[2], m[11]])
    re, im, c0, c1, norm = first_row(flat)
    a2 = (re[2], im[2])
    b0, b1, b2 = [(m[3 + k], m[12 + k]) for k in range(3)]
    x, y = cmul(b1, c0), cmul(b0, c1)
    u, v = cmul_conj(b0, c0), cmul_conj(b1, c1)
    w = cmul(a2, (u[0] + v[0], u[1] + v[1]))
    return flat + to_flat(
        x[0] - y[0], [x[1] - y[1], norm * b2[0] - w[0], norm * b2[1] - w[1]]
    )


def decode(values):
    re, im, c0, c1, norm = first_row(values[:5])
    p0, p1, r0, r1 = from_flat(values[5:])
    p, r = (p0, p1), (r0, r1)
    turn = cmul_conj(r, (re[2], im[2]))
    x, y = cmul_conj(p, c1), cmul(turn, c0)
    u, v = cmul_conj(p, c0), cmul(turn, c1)
    return third_row(
        re + [-x[0] - y[0], u[0] - v[0], norm * r0]
        + im + [-x[1] - y[1], u[1] - v[1], norm * r1]
    )


PAIRS = ((0, 1), (0, 2), (1, 2))


def kernel(
    sizes,
    links_hbm,
    trans_hbm,
    g,
    mon_out,
    links,
    w,
    cb,
    py,
    pz,
    tsend,
    trecv,
    halo,
    esend,
    erecv,
    zsend,
    zrecv,
    ysend,
    yrecv,
    mon,
    plane,
    load_sem,
    t_send_sem,
    t_recv_sem,
    first_send_sem,
    first_recv_sem,
    side_send_sem,
    side_recv_sem,
    red_send,
    red_recv,
):
    slices, depth, row_len = g.shape[2:]
    nh = row_len // LANES
    half = NX // 2
    strips = LANES // half
    groups = ysend.shape[3]
    last = slices - 1
    steps = 2 * ITERS
    me = {a: lax.axis_index(a) for a in AXES}

    def peer(axis, d):
        n = sizes[axis]
        return {axis: lax.rem(me[axis] + d + n, n)}

    loads = [
        pltpu.make_async_copy(src, dst, load_sem.at[number])
        for number, (src, dst) in enumerate(
            [
                (trans_hbm.at[1], g.at[1]),
                (links_hbm.at[1, 3], links.at[1, 3]),
                (links_hbm.at[1, pl.ds(1, 2)], links.at[1, pl.ds(1, 2)]),
                (trans_hbm.at[0], g.at[0]),
                (links_hbm.at[0, 3], links.at[0, 3]),
                (links_hbm.at[1, 0], links.at[1, 0]),
                (links_hbm.at[0, pl.ds(0, 3)], links.at[0, pl.ds(0, 3)]),
            ]
        )
    ]
    for copy in loads:
        copy.start()
    barrier = pltpu.get_barrier_semaphore()
    near = [(a, d) for a in AXES for d in sorted({1, sizes[a] - 1})]
    for axis, d in near:
        pl.semaphore_signal(barrier, inc=1, device_id=peer(axis, d), device_id_type=MESH)
    mon[...] = jnp.zeros_like(mon)
    pl.semaphore_wait(barrier, len(near))

    row = lax.broadcasted_iota(jnp.int32, (depth, LANES), 0)
    lane = lax.broadcasted_iota(jnp.int32, (depth, LANES), 1)
    column = lane % half
    strip = lane // half
    flip = 1 - lax.rem(me["ta"], 2)

    def piece(h):
        return pl.ds(h * LANES if isinstance(h, int) else pl.multiple_of(h * LANES, LANES), LANES)

    def load(ref, *index):
        t, h = index[-2:]
        return [ref[index[:-2] + (comp, t, slice(None), piece(h))] for comp in range(18)]

    def store(ref, values, *index):
        t, h = index[-2:]
        for comp in range(18):
            ref[index[:-2] + (comp, t, slice(None), piece(h))] = values[comp]

    def put(ref, index, h, values):
        for number, value in enumerate(values):
            ref[index + (number, slice(None), piece(h))] = value

    def get(ref, index, h, count):
        return [ref[index + (number, slice(None), piece(h))] for number in range(count)]

    def along_t(way):
        return {"ta": lax.rem(me["ta"] + 2 * way - 1 + sizes["ta"], sizes["ta"])}

    def t_copy(slot, way, h):
        return pltpu.make_async_remote_copy(
            src_ref=tsend.at[slot, way, :, :, piece(h)],
            dst_ref=trecv.at[slot, way, :, :, piece(h)],
            send_sem=t_send_sem.at[slot % 2, way, h],
            recv_sem=t_recv_sem.at[slot % 2, way, h],
            device_id=along_t(way),
            device_id_type=MESH,
        )

    def first_copy(colour, way, h):
        return pltpu.make_async_remote_copy(
            src_ref=esend.at[colour, way, :, :, piece(h)],
            dst_ref=erecv.at[colour, way, :, :, piece(h)],
            send_sem=first_send_sem.at[colour, way, h],
            recv_sem=first_recv_sem.at[colour, way, h],
            device_id=along_t(way),
            device_id_type=MESH,
        )

    def send_first(colour, way, h):
        values = load(g, colour, last if way else 0, h)
        if way:
            values = mul(values, load(links, colour, 3, last, h))
        put(esend, (colour, way), h, encode(values))
        first_copy(colour, way, h).start()

    def take_first(colour, way, h):
        first_copy(colour, way, h).wait()
        m = decode(get(erecv, (colour, way), h, 8))
        put(halo, (colour, way), h, m)
        return m

    def side(k, t):
        ends = [(zsend, zrecv, "gz"), (ysend, yrecv, "gy")]
        return [
            pltpu.make_async_remote_copy(
                src_ref=src.at[k, way, t],
                dst_ref=dst.at[k, way, t],
                send_sem=side_send_sem.at[k % 2, 2 * number + way, t],
                recv_sem=side_recv_sem.at[k % 2, 2 * number + way, t],
                device_id=peer(axis, 1 if way else -1),
                device_id_type=MESH,
            )
            for number, (src, dst, axis) in enumerate(ends)
            for way in range(2)
        ]

    def pack(values, ref, k, way, t):
        for group in range(groups):
            tile = None
            for j in range(strips):
                comp = group * strips + j
                if comp >= 18:
                    continue
                turn = (half * (j + way)) % LANES
                moved = pltpu.roll(values[comp], turn, 1) if turn else values[comp]
                tile = moved if tile is None else jnp.where(strip == j, moved, tile)
            ref[k, way, t, group] = tile

    def unpack(ref, k, way, t):
        out = []
        for comp in range(18):
            group, j = comp // strips, comp % strips
            tile = ref[k, way, t, group]
            turn = (LANES - half - half * j if way == 0 else LANES - half * j) % LANES
            out.append(pltpu.roll(tile, turn, 1) if turn else tile)
        return out

    def products(k, p, t, h, other):
        prod_y = mul(other, load(links, p, 1, t, h))
        store(py, prod_y, t, h)
        if h == 0:
            pack(other, ysend, k, 0, t)
        if h == nh - 1:
            pack(prod_y, ysend, k, 1, t)
        prod_z = mul(other, load(links, p, 2, t, h))
        store(pz, prod_z, t, h)
        for comp in range(18):
            zsend[k, 0, t, comp : comp + 1, piece(h)] = other[comp][0:1]
            zsend[k, 1, t, comp : comp + 1, piece(h)] = prod_z[comp][depth - 1 : depth]

    def turn_own(k, c, t, way, h):
        own = turn(load(g, c, t, h), get(tsend, (k, way), h, 11))
        store(g, own, c, t, h)
        return own

    def half_sweep(n, c):
        p = 1 - c
        k = 2 * n + c
        if c == 0:
            @pl.when(n == 0)
            def _():
                for copy in loads[5:]:
                    copy.wait()

        def inside(h, _):
            for t in range(slices):
                offset = (row + strip + (t + c)) % 2
                other = load(g, p, t, h)
                ahead = []
                for v in other:
                    stepped = jnp.where(
                        column == half - 1, pltpu.roll(v, half - 1, 1), pltpu.roll(v, LANES - 1, 1)
                    )
                    ahead.append(jnp.where(offset == 0, v, stepped))
                acc = mul_adj(load(links, c, 0, t, h), ahead)
                behind = []
                for v in mul(other, load(links, p, 0, t, h)):
                    stepped = jnp.where(
                        column == 0, pltpu.roll(v, LANES - half + 1, 1), pltpu.roll(v, 1, 1)
                    )
                    behind.append(jnp.where(offset == 0, stepped, v))
                acc = add_adj(acc, behind)
                if t < last:
                    acc = add(acc, mul_adj(load(links, c, 3, t, h), load(g, p, t + 1, h)))
                if t > 0:
                    acc = add_adj(acc, mul(load(g, p, t - 1, h), load(links, p, 3, t - 1, h)))
                store(w, acc, t, h)

            def outer():
                return (
                    mul(load(g, c, last, h), load(links, c, 3, last, h)),
                    load(g, c, 0, h),
                )

            def turned_halo(way):
                m = turn(get(halo, (p, way), h, 18), get(trecv, (k - 3, way), h, 11))
                put(halo, (p, way), h, m)
                return m

            def prepare(*halos):
                for way, values in enumerate(outer()):
                    if halos:
                        values = mul_adj(halos[0](way), values)
                    put(cb, (way,), h, values)

            if c == 0:
                pl.when(n == 0)(lambda: prepare())
                pl.when(n == 1)(lambda: prepare(lambda way: get(halo, (p, way), h, 18)))
                if ITERS > 2:
                    pl.when(n > 1)(lambda: prepare(turned_halo))
            else:
                pl.when(n == 0)(lambda: prepare(lambda way: take_first(p, way, h)))
                pl.when(n > 0)(lambda: prepare(turned_halo))
            return 0

        lax.fori_loop(0, nh, inside, 0)

        def along_yz(t, h):
            acc = load(w, t, h)
            behind, ahead = [], []
            prod_z = load(pz, t, h)
            other = load(g, p, t, h)
            for comp in range(18):
                edge = zrecv[k, 0, t, comp : comp + 1, piece(h)]
                edge = jnp.broadcast_to(edge, (depth, LANES))
                moved = pltpu.roll(other[comp], depth - 1, 0)
                ahead.append(jnp.where(row == depth - 1, edge, moved))
                edge = zrecv[k, 1, t, comp : comp + 1, piece(h)]
                edge = jnp.broadcast_to(edge, (depth, LANES))
                behind.append(jnp.where(row == 0, edge, pltpu.roll(prod_z[comp], 1, 0)))
            acc = add_adj(acc, behind)
            acc = add(acc, mul_adj(load(links, c, 2, t, h), ahead))
            if h == nh - 1:
                edge = unpack(yrecv, k, 0, t)
            else:
                edge = [pltpu.roll(v, LANES - half, 1) for v in load(g, p, t, h + 1)]
            ahead = [
                jnp.where(strip == strips - 1, e, pltpu.roll(v, LANES - half, 1))
                for e, v in zip(edge, other)
            ]
            acc = add(acc, mul_adj(load(links, c, 1, t, h), ahead))
            if h == 0:
                edge = unpack(yrecv, k, 1, t)
            else:
                edge = [pltpu.roll(v, half, 1) for v in load(py, t, h - 1)]
            behind = [
                jnp.where(strip == 0, e, pltpu.roll(v, half, 1))
                for e, v in zip(edge, load(py, t, h))
            ]
            acc = add_adj(acc, behind)
            store(w, mul(load(g, c, t, h), acc), t, h)

        def take(way, h):
            def later():
                t_copy(k - 1, way, h).wait()
                m = turn(get(cb, (way,), h, 18), get(trecv, (k - 1, way), h, 11))
                put(cb, (way,), h, m)

            if c == 1:
                later()
                return

            @pl.when(n == 0)
            def _():
                put(cb, (way,), h, mul_adj(take_first(p, way, h), get(cb, (way,), h, 18)))

            pl.when(n > 0)(later)

        def monitor(a):
            func = a[0] + a[4] + a[8]
            mean = (a[9] + a[13] + a[17]) * (1.0 / 3.0)
            div = None
            for i in range(3):
                d = a[9 + 4 * i] - mean
                div = d * d if div is None else div + d * d
            for i, j in PAIRS:
                d = a[3 * i + j] - a[3 * j + i]
                e = a[9 + 3 * i + j] + a[9 + 3 * j + i]
                div = div + 0.5 * (d * d + e * e)
            mon[n, 0] += func
            mon[n, 1] += div

        def slab(number, _):
            back = (number + flip) % 2
            ahead = 1 - back
            t = ahead * last
            for copy in side(k, t):
                copy.wait()
            for h in range(nh):
                along_yz(t, h)
            for h in range(nh):
                take(back, h)
                a = add_adj(load(w, t, h), get(cb, (back,), h, 18))
                turns = []
                for i, j in PAIRS:
                    q = rotation(a, i, j)
                    turns.append(q)
                    a = rotate(a, q, i, j)
                put(tsend, (k, ahead), h, reduced(*turns))

                if c == 0:
                    t_copy(k, ahead, h).start()
                    products(k + 1, c, t, h, turn_own(k, c, t, ahead, h))
                else:
                    @pl.when(k + 1 < steps)
                    def _():
                        t_copy(k, ahead, h).start()

                    monitor(a)

                    @pl.when(k + 1 < steps)
                    def _():
                        products(k + 1, c, t, h, turn_own(k, c, t, ahead, h))

            def follow():
                for copy in side(k + 1, t):
                    copy.start()

            if c == 0:
                follow()
            else:
                pl.when(k + 1 < steps)(follow)
            return 0

        lax.fori_loop(0, slices, slab, 0)

    def send_both(colour):
        for order in range(2):
            @pl.when(flip == 1 - order)
            def _():
                for way in (order, 1 - order):
                    for h in range(nh):
                        send_first(colour, way, h)

    loads[0].wait()
    loads[1].wait()
    send_both(1)
    loads[2].wait()
    for t in range(slices):
        for h in range(nh):
            products(0, 1, t, h, load(g, 1, t, h))
        for copy in side(0, t):
            copy.start()

    loads[3].wait()
    loads[4].wait()
    send_both(0)

    def iteration(n, _):
        half_sweep(n, 0)
        half_sweep(n, 1)
        return 0

    lax.fori_loop(0, ITERS, iteration, 0)

    spot = lax.broadcasted_iota(jnp.int32, (1, LANES), 1)
    sums = jnp.zeros((1, LANES), jnp.float32)
    for n in range(ITERS):
        for part in range(2):
            value = jnp.sum(jnp.sum(mon[n, part], axis=0, keepdims=True), axis=1, keepdims=True)
            sums = jnp.where(spot == 2 * n + part, value, sums)

    lines = plane.shape[0]
    here = (me["ta"] * sizes["gz"] + me["gz"]) * sizes["gy"] + me["gy"]
    plane[here] = sums
    offsets = [
        (i, j, k)
        for i in range(sizes["ta"])
        for j in range(sizes["gz"])
        for k in range(sizes["gy"])
        if i or j or k
    ]

    toward = 1 - 2 * (2 * me["ta"] // sizes["ta"])

    def to_other(i, j, k):
        return pltpu.make_async_remote_copy(
            src_ref=plane.at[here],
            dst_ref=plane.at[here],
            send_sem=red_send,
            recv_sem=red_recv,
            device_id=peer("ta", i) | peer("gz", j) | peer("gy", k),
            device_id_type=MESH,
        )

    for offset in reversed(offsets):
        to_other(*offset).start()
    width = sizes["gz"] * sizes["gy"]
    arrivals = pltpu.make_async_remote_copy(
        src_ref=plane.at[pl.ds(0, lines - 1)],
        dst_ref=plane.at[pl.ds(0, lines - 1)],
        send_sem=red_send,
        recv_sem=red_recv,
        device_id=peer("ta", 1),
        device_id_type=MESH,
    )
    for t in range(slices):
        for h in range(nh):
            turn_own(steps - 1, 1, t, t, h)
    arrivals.wait_send()
    arrivals.wait_recv()
    sums = total([plane[number] for number in range(lines)])
    sites = slices * depth * row_len * sizes["ta"] * width
    for n in range(ITERS):
        mon_out[0, n] = 1.0 - sums[0, 2 * n] / (24.0 * sites)
        mon_out[1, n] = sums[0, 2 * n + 1] / float(sites)


def shards(sizes, lattice_links, transform):
    slices, depth, row_len = transform.shape[2:]
    nh = row_len // LANES
    strips = LANES // (NX // 2)
    groups = -(-18 // strips)
    steps = 2 * ITERS
    face = (18, slices, depth, row_len)
    assert depth == 8 and slices == 2 and row_len % LANES == 0
    f32 = jnp.float32
    width = sizes["gz"] * sizes["gy"]
    lines = width * sizes["ta"]
    g, mon = pl.pallas_call(
        functools.partial(kernel, sizes),
        out_shape=(
            pltpu.VMEM(transform.shape, f32),
            pltpu.SMEM((2, ITERS), f32),
        ),
        in_specs=[pl.BlockSpec(memory_space=pltpu.HBM)] * 2,
        out_specs=(
            pl.BlockSpec(memory_space=pltpu.VMEM),
            pl.BlockSpec(memory_space=pltpu.SMEM),
        ),
        scratch_shapes=[
            pltpu.VMEM(lattice_links.shape, f32),
            pltpu.VMEM(face, f32),
            pltpu.VMEM((2, 18, depth, row_len), f32),
            pltpu.VMEM(face, f32),
            pltpu.VMEM(face, f32),
            pltpu.VMEM((steps, 2, 11, depth, row_len), f32),
            pltpu.VMEM((steps, 2, 11, depth, row_len), f32),
            pltpu.VMEM((2, 2, 18, depth, row_len), f32),
            pltpu.VMEM((2, 2, 8, depth, row_len), f32),
            pltpu.VMEM((2, 2, 8, depth, row_len), f32),
            pltpu.VMEM((steps, 2, slices, 18, row_len), f32),
            pltpu.VMEM((steps, 2, slices, 18, row_len), f32),
            pltpu.VMEM((steps, 2, slices, groups, depth, LANES), f32),
            pltpu.VMEM((steps, 2, slices, groups, depth, LANES), f32),
            pltpu.VMEM((ITERS, 2, depth, LANES), f32),
            pltpu.VMEM((lines, 1, LANES), f32),
            pltpu.SemaphoreType.DMA((7,)),
            pltpu.SemaphoreType.DMA((2, 2, nh)),
            pltpu.SemaphoreType.DMA((2, 2, nh)),
            pltpu.SemaphoreType.DMA((2, 2, nh)),
            pltpu.SemaphoreType.DMA((2, 2, nh)),
            pltpu.SemaphoreType.DMA((2, 4, slices)),
            pltpu.SemaphoreType.DMA((2, 4, slices)),
            pltpu.SemaphoreType.DMA,
            pltpu.SemaphoreType.DMA,
        ],
        compiler_params=pltpu.CompilerParams(
            collective_id=0, has_side_effects=True, vmem_limit_bytes=67043328 - 900000 // 4096 * 4096
        ),
    )(lattice_links, transform)

    def finish(g_ref, mon_ref, out_ref, mon_out, sem, sem2):
        copy = pltpu.make_async_copy(g_ref, out_ref, sem)
        copy.start()
        small = pltpu.make_async_copy(mon_ref, mon_out, sem2)
        small.start()
        copy.wait()
        small.wait()

    return pl.pallas_call(
        finish,
        out_shape=(
            jax.ShapeDtypeStruct(transform.shape, f32),
            jax.ShapeDtypeStruct((2, ITERS), f32),
        ),
        in_specs=[pl.BlockSpec(memory_space=pltpu.VMEM), pl.BlockSpec(memory_space=pltpu.SMEM)],
        out_specs=(pl.BlockSpec(memory_space=pltpu.HBM), pl.BlockSpec(memory_space=pltpu.HBM)),
        scratch_shapes=[pltpu.SemaphoreType.DMA,pltpu.SemaphoreType.DMA],
        compiler_params=pltpu.CompilerParams(vmem_limit_bytes=1 << 20),
    )(g, mon)


def solution(mesh):
    sizes = {axis: mesh.shape[axis] for axis in AXES}
    return jax.shard_map(
        functools.partial(shards, sizes),
        mesh=mesh,
        in_specs=(P(None, None, None, "ta", "gz", "gy"), P(None, None, "ta", "gz", "gy")),
        out_specs=(P(None, None, "ta", "gz", "gy"), P()),
        check_vma=False,
    )
```

```python
import functools

import jax
import jax.numpy as jnp
from jax import lax
from jax.experimental import pallas as pl
from jax.experimental.pallas import tpu as pltpu
from jax.sharding import PartitionSpec as P

NX = 64
ITERS = 2
OMEGA = 1.7
GUARD = 1e-12
FLOOR = 1e-20
FAR = 1e15
LANES = 128
AXES = ("ta", "gz", "gy")
MESH = pl.DeviceIdType.MESH


def total(terms):
    out = terms[0]
    for term in terms[1:]:
        out = out + term
    return out


def mul(a, b):
    re, im = [], []
    for i in range(3):
        for j in range(3):
            re.append(
                total([a[3 * i + k] * b[3 * k + j] for k in range(3)])
                - total([a[9 + 3 * i + k] * b[9 + 3 * k + j] for k in range(3)])
            )
            im.append(
                total([a[3 * i + k] * b[9 + 3 * k + j] for k in range(3)])
                + total([a[9 + 3 * i + k] * b[3 * k + j] for k in range(3)])
            )
    return re + im


def mul_adj(a, b):
    re, im = [], []
    for i in range(3):
        for j in range(3):
            re.append(
                total([a[3 * i + k] * b[3 * j + k] for k in range(3)])
                + total([a[9 + 3 * i + k] * b[9 + 3 * j + k] for k in range(3)])
            )
            im.append(
                total([a[9 + 3 * i + k] * b[3 * j + k] for k in range(3)])
                - total([a[3 * i + k] * b[9 + 3 * j + k] for k in range(3)])
            )
    return re + im


def add(a, b):
    return [x + y for x, y in zip(a, b)]


def add_adj(a, b):
    out = []
    for i in range(3):
        for j in range(3):
            out.append(a[3 * i + j] + b[3 * j + i])
    for i in range(3):
        for j in range(3):
            out.append(a[9 + 3 * i + j] - b[9 + 3 * j + i])
    return out


def rotation(a, i, j):
    ii, jj, ij, ji = 4 * i, 4 * j, 3 * i + j, 3 * j + i
    v0 = a[ii] + a[jj]
    v1 = -(a[9 + ij] + a[9 + ji])
    v2 = a[ji] - a[ij]
    v3 = a[9 + jj] - a[9 + ii]
    tail = v1 * v1 + v2 * v2 + v3 * v3
    length = jnp.sqrt(v0 * v0 + tail)
    s0 = (1.0 - OMEGA) * length + OMEGA * v0
    inv = lax.rsqrt(s0 * s0 + (OMEGA * OMEGA) * tail + GUARD)
    scaled = OMEGA * inv
    return (s0 * inv, v1 * scaled, v2 * scaled, v3 * scaled)


def rotate(m, q, i, j):
    q0, q1, q2 = q[:3]
    out = list(m)
    for k in range(3):
        ur, ui = m[3 * i + k], m[9 + 3 * i + k]
        lr, li = m[3 * j + k], m[9 + 3 * j + k]
        values = [
            q0 * ur + q2 * lr - q1 * li,
            q0 * ui + q2 * li + q1 * lr,
            q0 * lr - q2 * ur - q1 * ui,
            q0 * li - q2 * ui + q1 * ur,
        ]
        if len(q) == 4:
            turned = [-ui, ur, li, -lr]
            values = [v + q[3] * u for v, u in zip(values, turned)]
        out[3 * i + k], out[9 + 3 * i + k] = values[:2]
        out[3 * j + k], out[9 + 3 * j + k] = values[2:]
    return out


PARTS = (slice(0, 3), slice(3, 7), slice(7, 11))


def turn(m, q):
    for part, (i, j) in zip(PARTS, PAIRS):
        m = rotate(m, q[part], i, j)
    return m


def reduced(first, second, third):
    r0, r1, r2, r3 = first
    square = r0 * r0 + r3 * r3
    small = square < FLOOR
    inv = lax.rsqrt(jnp.where(small, 1.0, square))
    phase = (jnp.where(small, 1.0, r0 * inv), jnp.where(small, 0.0, -r3 * inv))
    back = (phase[0], -phase[1])
    a2, a1 = cmul(phase, (r2, r1))
    b0, b3 = cmul(back, (second[0], second[3]))
    c0, c3 = cmul(phase, (third[0], third[3]))
    c2, c1 = cmul(back, (third[2], third[1]))
    return [square * inv, a1, a2, b0, second[1], second[2], b3, c0, c1, c2, c3]


def third_row(m):
    re, im = list(m[:6]), list(m[6:])
    for k in range(3):
        a, b = (k + 1) % 3, (k + 2) % 3
        re.append(
            m[a] * m[3 + b] - m[6 + a] * m[9 + b] - m[b] * m[3 + a] + m[6 + b] * m[9 + a]
        )
        im.append(
            m[b] * m[9 + a] + m[6 + b] * m[3 + a] - m[a] * m[9 + b] - m[6 + a] * m[3 + b]
        )
    return re + im


def to_flat(x, v):
    square = total([c * c for c in v])
    scale = jnp.where(x >= 0.0, 1.0 + x, square / (1.0 + jnp.abs(x)))
    pole = scale < FLOOR
    inv = 1.0 / jnp.where(pole, 1.0, scale)
    flat = [c * inv for c in v]
    return [jnp.where(pole, FAR, flat[0])] + [jnp.where(pole, 0.0, c) for c in flat[1:]]


def from_flat(flat):
    scale = 2.0 / (1.0 + total([c * c for c in flat]))
    return [scale - 1.0] + [c * scale for c in flat]


def cmul(a, b):
    return (a[0] * b[0] - a[1] * b[1], a[0] * b[1] + a[1] * b[0])


def cmul_conj(a, b):
    return (a[0] * b[0] + a[1] * b[1], a[1] * b[0] - a[0] * b[1])


def first_row(flat):
    r0, i0, r1, i1, r2, i2 = from_flat(flat)
    square = r0 * r0 + i0 * i0 + r1 * r1 + i1 * i1
    small = square < FLOOR
    inv = lax.rsqrt(jnp.where(small, 1.0, square))
    c0 = (jnp.where(small, 1.0, r0 * inv), jnp.where(small, 0.0, i0 * inv))
    c1 = (jnp.where(small, 0.0, r1 * inv), jnp.where(small, 0.0, i1 * inv))
    norm = jnp.where(small, 0.0, square * inv)
    return [r0, r1, r2], [i0, i1, i2], c0, c1, norm


def encode(m):
    flat = to_flat(m[0], [m[9], m[1], m[10], m[2], m[11]])
    re, im, c0, c1, norm = first_row(flat)
    a2 = (re[2], im[2])
    b0, b1, b2 = [(m[3 + k], m[12 + k]) for k in range(3)]
    x, y = cmul(b1, c0), cmul(b0, c1)
    u, v = cmul_conj(b0, c0), cmul_conj(b1, c1)
    w = cmul(a2, (u[0] + v[0], u[1] + v[1]))
    return flat + to_flat(
        x[0] - y[0], [x[1] - y[1], norm * b2[0] - w[0], norm * b2[1] - w[1]]
    )


def decode(values):
    re, im, c0, c1, norm = first_row(values[:5])
    p0, p1, r0, r1 = from_flat(values[5:])
    p, r = (p0, p1), (r0, r1)
    turn = cmul_conj(r, (re[2], im[2]))
    x, y = cmul_conj(p, c1), cmul(turn, c0)
    u, v = cmul_conj(p, c0), cmul(turn, c1)
    return third_row(
        re + [-x[0] - y[0], u[0] - v[0], norm * r0]
        + im + [-x[1] - y[1], u[1] - v[1], norm * r1]
    )


PAIRS = ((0, 1), (0, 2), (1, 2))


def kernel(
    sizes,
    links_hbm,
    trans_hbm,
    g,
    mon_out,
    links,
    w,
    cb,
    py,
    pz,
    tsend,
    trecv,
    halo,
    esend,
    erecv,
    zsend,
    zrecv,
    ysend,
    yrecv,
    mon,
    plane,
    load_sem,
    t_send_sem,
    t_recv_sem,
    first_send_sem,
    first_recv_sem,
    side_send_sem,
    side_recv_sem,
    red_send,
    red_recv,
):
    slices, depth, row_len = g.shape[2:]
    nh = row_len // LANES
    half = NX // 2
    strips = LANES // half
    groups = ysend.shape[3]
    last = slices - 1
    steps = 2 * ITERS
    me = {a: lax.axis_index(a) for a in AXES}

    def peer(axis, d):
        n = sizes[axis]
        return {axis: lax.rem(me[axis] + d + n, n)}

    loads = [
        pltpu.make_async_copy(src, dst, load_sem.at[number])
        for number, (src, dst) in enumerate(
            [
                (trans_hbm.at[1], g.at[1]),
                (links_hbm.at[1, 3], links.at[1, 3]),
                (links_hbm.at[1, pl.ds(1, 2)], links.at[1, pl.ds(1, 2)]),
                (trans_hbm.at[0], g.at[0]),
                (links_hbm.at[0, 3], links.at[0, 3]),
                (links_hbm.at[1, 0], links.at[1, 0]),
                (links_hbm.at[0, pl.ds(0, 3)], links.at[0, pl.ds(0, 3)]),
            ]
        )
    ]
    for copy in loads:
        copy.start()
    barrier = pltpu.get_barrier_semaphore()
    near = [(a, d) for a in AXES for d in sorted({1, sizes[a] - 1})]
    for axis, d in near:
        pl.semaphore_signal(barrier, inc=1, device_id=peer(axis, d), device_id_type=MESH)
    mon[...] = jnp.zeros_like(mon)
    pl.semaphore_wait(barrier, len(near))

    row = lax.broadcasted_iota(jnp.int32, (depth, LANES), 0)
    lane = lax.broadcasted_iota(jnp.int32, (depth, LANES), 1)
    column = lane % half
    strip = lane // half
    flip = 1 - lax.rem(me["ta"], 2)

    def piece(h):
        return pl.ds(h * LANES if isinstance(h, int) else pl.multiple_of(h * LANES, LANES), LANES)

    def load(ref, *index):
        t, h = index[-2:]
        return [ref[index[:-2] + (comp, t, slice(None), piece(h))] for comp in range(18)]

    def store(ref, values, *index):
        t, h = index[-2:]
        for comp in range(18):
            ref[index[:-2] + (comp, t, slice(None), piece(h))] = values[comp]

    def put(ref, index, h, values):
        for number, value in enumerate(values):
            ref[index + (number, slice(None), piece(h))] = value

    def get(ref, index, h, count):
        return [ref[index + (number, slice(None), piece(h))] for number in range(count)]

    def along_t(way):
        return {"ta": lax.rem(me["ta"] + 2 * way - 1 + sizes["ta"], sizes["ta"])}

    def t_copy(slot, way, h):
        return pltpu.make_async_remote_copy(
            src_ref=tsend.at[slot, way, :, :, piece(h)],
            dst_ref=trecv.at[slot, way, :, :, piece(h)],
            send_sem=t_send_sem.at[slot % 2, way, h],
            recv_sem=t_recv_sem.at[slot % 2, way, h],
            device_id=along_t(way),
            device_id_type=MESH,
        )

    def first_copy(colour, way, h):
        return pltpu.make_async_remote_copy(
            src_ref=esend.at[colour, way, :, :, piece(h)],
            dst_ref=erecv.at[colour, way, :, :, piece(h)],
            send_sem=first_send_sem.at[colour, way, h],
            recv_sem=first_recv_sem.at[colour, way, h],
            device_id=along_t(way),
            device_id_type=MESH,
        )

    def send_first(colour, way, h):
        values = load(g, colour, last if way else 0, h)
        if way:
            values = mul(values, load(links, colour, 3, last, h))
        put(esend, (colour, way), h, encode(values))
        first_copy(colour, way, h).start()

    def take_first(colour, way, h):
        first_copy(colour, way, h).wait()
        m = decode(get(erecv, (colour, way), h, 8))
        put(halo, (colour, way), h, m)
        return m

    def side(k, t):
        ends = [(zsend, zrecv, "gz"), (ysend, yrecv, "gy")]
        return [
            pltpu.make_async_remote_copy(
                src_ref=src.at[k, way, t],
                dst_ref=dst.at[k, way, t],
                send_sem=side_send_sem.at[k % 2, 2 * number + way, t],
                recv_sem=side_recv_sem.at[k % 2, 2 * number + way, t],
                device_id=peer(axis, 1 if way else -1),
                device_id_type=MESH,
            )
            for number, (src, dst, axis) in enumerate(ends)
            for way in range(2)
        ]

    def pack(values, ref, k, way, t):
        for group in range(groups):
            tile = None
            for j in range(strips):
                comp = group * strips + j
                if comp >= 18:
                    continue
                turn = (half * (j + way)) % LANES
                moved = pltpu.roll(values[comp], turn, 1) if turn else values[comp]
                tile = moved if tile is None else jnp.where(strip == j, moved, tile)
            ref[k, way, t, group] = tile

    def unpack(ref, k, way, t):
        out = []
        for comp in range(18):
            group, j = comp // strips, comp % strips
            tile = ref[k, way, t, group]
            turn = (LANES - half - half * j if way == 0 else LANES - half * j) % LANES
            out.append(pltpu.roll(tile, turn, 1) if turn else tile)
        return out

    def products(k, p, t, h, other):
        prod_y = mul(other, load(links, p, 1, t, h))
        store(py, prod_y, t, h)
        if h == 0:
            pack(other, ysend, k, 0, t)
        if h == nh - 1:
            pack(prod_y, ysend, k, 1, t)
        prod_z = mul(other, load(links, p, 2, t, h))
        store(pz, prod_z, t, h)
        for comp in range(18):
            zsend[k, 0, t, comp : comp + 1, piece(h)] = other[comp][0:1]
            zsend[k, 1, t, comp : comp + 1, piece(h)] = prod_z[comp][depth - 1 : depth]

    def turn_own(k, c, t, way, h):
        own = turn(load(g, c, t, h), get(tsend, (k, way), h, 11))
        store(g, own, c, t, h)
        return own

    def half_sweep(n, c):
        p = 1 - c
        k = 2 * n + c
        if c == 0:
            @pl.when(n == 0)
            def _():
                for copy in loads[5:]:
                    copy.wait()

        def inside(h, _):
            for t in range(slices):
                offset = (row + strip + (t + c)) % 2
                other = load(g, p, t, h)
                ahead = []
                for v in other:
                    stepped = jnp.where(
                        column == half - 1, pltpu.roll(v, half - 1, 1), pltpu.roll(v, LANES - 1, 1)
                    )
                    ahead.append(jnp.where(offset == 0, v, stepped))
                acc = mul_adj(load(links, c, 0, t, h), ahead)
                behind = []
                for v in mul(other, load(links, p, 0, t, h)):
                    stepped = jnp.where(
                        column == 0, pltpu.roll(v, LANES - half + 1, 1), pltpu.roll(v, 1, 1)
                    )
                    behind.append(jnp.where(offset == 0, stepped, v))
                acc = add_adj(acc, behind)
                if t < last:
                    acc = add(acc, mul_adj(load(links, c, 3, t, h), load(g, p, t + 1, h)))
                if t > 0:
                    acc = add_adj(acc, mul(load(g, p, t - 1, h), load(links, p, 3, t - 1, h)))
                store(w, acc, t, h)

            def outer():
                return (
                    mul(load(g, c, last, h), load(links, c, 3, last, h)),
                    load(g, c, 0, h),
                )

            def turned_halo(way):
                m = turn(get(halo, (p, way), h, 18), get(trecv, (k - 3, way), h, 11))
                put(halo, (p, way), h, m)
                return m

            def prepare(*halos):
                for way, values in enumerate(outer()):
                    if halos:
                        values = mul_adj(halos[0](way), values)
                    put(cb, (way,), h, values)

            if c == 0:
                pl.when(n == 0)(lambda: prepare())
                pl.when(n == 1)(lambda: prepare(lambda way: get(halo, (p, way), h, 18)))
                if ITERS > 2:
                    pl.when(n > 1)(lambda: prepare(turned_halo))
            else:
                pl.when(n == 0)(lambda: prepare(lambda way: take_first(p, way, h)))
                pl.when(n > 0)(lambda: prepare(turned_halo))
            return 0

        lax.fori_loop(0, nh, inside, 0)

        def along_yz(t, h):
            acc = load(w, t, h)
            behind, ahead = [], []
            prod_z = load(pz, t, h)
            other = load(g, p, t, h)
            for comp in range(18):
                edge = zrecv[k, 0, t, comp : comp + 1, piece(h)]
                edge = jnp.broadcast_to(edge, (depth, LANES))
                moved = pltpu.roll(other[comp], depth - 1, 0)
                ahead.append(jnp.where(row == depth - 1, edge, moved))
                edge = zrecv[k, 1, t, comp : comp + 1, piece(h)]
                edge = jnp.broadcast_to(edge, (depth, LANES))
                behind.append(jnp.where(row == 0, edge, pltpu.roll(prod_z[comp], 1, 0)))
            acc = add_adj(acc, behind)
            acc = add(acc, mul_adj(load(links, c, 2, t, h), ahead))
            if h == nh - 1:
                edge = unpack(yrecv, k, 0, t)
            else:
                edge = [pltpu.roll(v, LANES - half, 1) for v in load(g, p, t, h + 1)]
            ahead = [
                jnp.where(strip == strips - 1, e, pltpu.roll(v, LANES - half, 1))
                for e, v in zip(edge, other)
            ]
            acc = add(acc, mul_adj(load(links, c, 1, t, h), ahead))
            if h == 0:
                edge = unpack(yrecv, k, 1, t)
            else:
                edge = [pltpu.roll(v, half, 1) for v in load(py, t, h - 1)]
            behind = [
                jnp.where(strip == 0, e, pltpu.roll(v, half, 1))
                for e, v in zip(edge, load(py, t, h))
            ]
            acc = add_adj(acc, behind)
            store(w, mul(load(g, c, t, h), acc), t, h)

        def take(way, h):
            def later():
                t_copy(k - 1, way, h).wait()
                m = turn(get(cb, (way,), h, 18), get(trecv, (k - 1, way), h, 11))
                put(cb, (way,), h, m)

            if c == 1:
                later()
                return

            @pl.when(n == 0)
            def _():
                put(cb, (way,), h, mul_adj(take_first(p, way, h), get(cb, (way,), h, 18)))

            pl.when(n > 0)(later)

        def monitor(a):
            func = a[0] + a[4] + a[8]
            mean = (a[9] + a[13] + a[17]) * (1.0 / 3.0)
            div = None
            for i in range(3):
                d = a[9 + 4 * i] - mean
                div = d * d if div is None else div + d * d
            for i, j in PAIRS:
                d = a[3 * i + j] - a[3 * j + i]
                e = a[9 + 3 * i + j] + a[9 + 3 * j + i]
                div = div + 0.5 * (d * d + e * e)
            mon[n, 0] += func
            mon[n, 1] += div

        def slab(number, _):
            back = (number + flip) % 2
            ahead = 1 - back
            t = ahead * last
            for copy in side(k, t):
                copy.wait()
            for h in range(nh):
                along_yz(t, h)
            for h in range(nh):
                take(back, h)
                a = add_adj(load(w, t, h), get(cb, (back,), h, 18))
                turns = []
                for i, j in PAIRS:
                    q = rotation(a, i, j)
                    turns.append(q)
                    a = rotate(a, q, i, j)
                put(tsend, (k, ahead), h, reduced(*turns))

                if c == 0:
                    t_copy(k, ahead, h).start()
                    products(k + 1, c, t, h, turn_own(k, c, t, ahead, h))
                else:
                    @pl.when(k + 1 < steps)
                    def _():
                        t_copy(k, ahead, h).start()

                    monitor(a)

                    @pl.when(k + 1 < steps)
                    def _():
                        products(k + 1, c, t, h, turn_own(k, c, t, ahead, h))

            def follow():
                for copy in side(k + 1, t):
                    copy.start()

            if c == 0:
                follow()
            else:
                pl.when(k + 1 < steps)(follow)
            return 0

        lax.fori_loop(0, slices, slab, 0)

    def send_both(colour):
        for order in range(2):
            @pl.when(flip == 1 - order)
            def _():
                for way in (order, 1 - order):
                    for h in range(nh):
                        send_first(colour, way, h)

    loads[0].wait()
    loads[1].wait()
    send_both(1)
    loads[2].wait()
    for t in range(slices):
        for h in range(nh):
            products(0, 1, t, h, load(g, 1, t, h))
        for copy in side(0, t):
            copy.start()

    loads[3].wait()
    loads[4].wait()
    send_both(0)

    def iteration(n, _):
        half_sweep(n, 0)
        half_sweep(n, 1)
        return 0

    lax.fori_loop(0, ITERS, iteration, 0)

    spot = lax.broadcasted_iota(jnp.int32, (1, LANES), 1)
    sums = jnp.zeros((1, LANES), jnp.float32)
    for n in range(ITERS):
        for part in range(2):
            value = jnp.sum(jnp.sum(mon[n, part], axis=0, keepdims=True), axis=1, keepdims=True)
            sums = jnp.where(spot == 2 * n + part, value, sums)

    lines = plane.shape[0]
    here = (me["ta"] * sizes["gz"] + me["gz"]) * sizes["gy"] + me["gy"]
    plane[here] = sums
    offsets = [
        (i, j, k)
        for i in range(sizes["ta"])
        for j in range(sizes["gz"])
        for k in range(sizes["gy"])
        if i or j or k
    ]

    toward = 1 - 2 * (2 * me["ta"] // sizes["ta"])

    def to_other(i, j, k):
        return pltpu.make_async_remote_copy(
            src_ref=plane.at[here],
            dst_ref=plane.at[here],
            send_sem=red_send,
            recv_sem=red_recv,
            device_id=peer("ta", i * toward) | peer("gz", j) | peer("gy", k),
            device_id_type=MESH,
        )

    for offset in reversed(offsets):
        to_other(*offset).start()
    width = sizes["gz"] * sizes["gy"]
    arrivals = pltpu.make_async_remote_copy(
        src_ref=plane.at[pl.ds(0, lines - 1)],
        dst_ref=plane.at[pl.ds(0, lines - 1)],
        send_sem=red_send,
        recv_sem=red_recv,
        device_id=peer("ta", 1),
        device_id_type=MESH,
    )
    for t in range(slices):
        for h in range(nh):
            turn_own(steps - 1, 1, t, t, h)
    arrivals.wait_send()
    arrivals.wait_recv()
    sums = total([plane[number] for number in range(lines)])
    sites = slices * depth * row_len * sizes["ta"] * width
    for n in range(ITERS):
        mon_out[0, n] = 1.0 - sums[0, 2 * n] / (24.0 * sites)
        mon_out[1, n] = sums[0, 2 * n + 1] / float(sites)


def shards(sizes, lattice_links, transform):
    slices, depth, row_len = transform.shape[2:]
    nh = row_len // LANES
    strips = LANES // (NX // 2)
    groups = -(-18 // strips)
    steps = 2 * ITERS
    face = (18, slices, depth, row_len)
    assert depth == 8 and slices == 2 and row_len % LANES == 0
    f32 = jnp.float32
    width = sizes["gz"] * sizes["gy"]
    lines = width * sizes["ta"]
    g, mon = pl.pallas_call(
        functools.partial(kernel, sizes),
        out_shape=(
            pltpu.VMEM(transform.shape, f32),
            pltpu.SMEM((2, ITERS), f32),
        ),
        in_specs=[pl.BlockSpec(memory_space=pltpu.HBM)] * 2,
        out_specs=(
            pl.BlockSpec(memory_space=pltpu.VMEM),
            pl.BlockSpec(memory_space=pltpu.SMEM),
        ),
        scratch_shapes=[
            pltpu.VMEM(lattice_links.shape, f32),
            pltpu.VMEM(face, f32),
            pltpu.VMEM((2, 18, depth, row_len), f32),
            pltpu.VMEM(face, f32),
            pltpu.VMEM(face, f32),
            pltpu.VMEM((steps, 2, 11, depth, row_len), f32),
            pltpu.VMEM((steps, 2, 11, depth, row_len), f32),
            pltpu.VMEM((2, 2, 18, depth, row_len), f32),
            pltpu.VMEM((2, 2, 8, depth, row_len), f32),
            pltpu.VMEM((2, 2, 8, depth, row_len), f32),
            pltpu.VMEM((steps, 2, slices, 18, row_len), f32),
            pltpu.VMEM((steps, 2, slices, 18, row_len), f32),
            pltpu.VMEM((steps, 2, slices, groups, depth, LANES), f32),
            pltpu.VMEM((steps, 2, slices, groups, depth, LANES), f32),
            pltpu.VMEM((ITERS, 2, depth, LANES), f32),
            pltpu.VMEM((lines, 1, LANES), f32),
            pltpu.SemaphoreType.DMA((7,)),
            pltpu.SemaphoreType.DMA((2, 2, nh)),
            pltpu.SemaphoreType.DMA((2, 2, nh)),
            pltpu.SemaphoreType.DMA((2, 2, nh)),
            pltpu.SemaphoreType.DMA((2, 2, nh)),
            pltpu.SemaphoreType.DMA((2, 4, slices)),
            pltpu.SemaphoreType.DMA((2, 4, slices)),
            pltpu.SemaphoreType.DMA,
            pltpu.SemaphoreType.DMA,
        ],
        compiler_params=pltpu.CompilerParams(
            collective_id=0, has_side_effects=True, vmem_limit_bytes=67043328 - 900000 // 4096 * 4096
        ),
    )(lattice_links, transform)

    def finish(g_ref, mon_ref, out_ref, mon_out, sem, sem2):
        copy = pltpu.make_async_copy(g_ref, out_ref, sem)
        copy.start()
        small = pltpu.make_async_copy(mon_ref, mon_out, sem2)
        small.start()
        copy.wait()
        small.wait()

    return pl.pallas_call(
        finish,
        out_shape=(
            jax.ShapeDtypeStruct(transform.shape, f32),
            jax.ShapeDtypeStruct((2, ITERS), f32),
        ),
        in_specs=[pl.BlockSpec(memory_space=pltpu.VMEM), pl.BlockSpec(memory_space=pltpu.SMEM)],
        out_specs=(pl.BlockSpec(memory_space=pltpu.HBM), pl.BlockSpec(memory_space=pltpu.HBM)),
        scratch_shapes=[pltpu.SemaphoreType.DMA,pltpu.SemaphoreType.DMA],
        compiler_params=pltpu.CompilerParams(vmem_limit_bytes=1 << 20),
    )(g, mon)


def solution(mesh):
    sizes = {axis: mesh.shape[axis] for axis in AXES}
    return jax.shard_map(
        functools.partial(shards, sizes),
        mesh=mesh,
        in_specs=(P(None, None, None, "ta", "gz", "gy"), P(None, None, "ta", "gz", "gy")),
        out_specs=(P(None, None, "ta", "gz", "gy"), P()),
        check_vma=False,
    )
```
